512 devices in a mesh: walkers: 128 (over z, y, x_hi), orb: 4 (over x_lo, core).
Axes of the slice: x: 4 (x_hi: 2, x_lo: 2; x = x_hi * 2 + x_lo), y: 8, z: 8, core: 2. Of those that a mesh axis runs over, the one named last changes fastest.
Arguments:
- inverse: float32 [512, 2, 128, 128], P('walkers', None, 'orb'), as said below
- slater: float32 [512, 2, 128, 128], P('walkers', None, 'orb'), may hold values from -1 to 3, as said below
- positions: float32 [512, 3, 256], P('walkers'), may hold values from -2 to 10
- displacements: float32 [512, 3, 256], P('walkers'), may hold values from -0.6 to 0.6
- move_order: int32 [512, 2, 128], P('walkers'), may hold values from 0 to 127, each once within a row
- accepted: int32 [512, 2, 32], P('walkers'), may hold values 0 or 1
- counts: int32 [512], P('walkers'), may hold values from 0 to 2, as said below
- log_amp: float32 [512], P('walkers'), may hold values from -4 to 4
- centers: float32 [3, 1024], replicated, may hold values from 0 to 8
- exponents: float32 [1024], replicated, may hold values from 0.3 to 3
- orbitals: float32 [2, 128, 1024], P(None, 'orb'), may hold values from -0.36 to 0.36
- jastrow: float32 [4], replicated, may hold values from 0.2 to 0.6
Outputs:
- inverse_new: float32 [512, 2, 128, 128], P('walkers', None, 'orb')
- slater_new: float32 [512, 2, 128, 128], P('walkers', None, 'orb')
- positions_new: float32 [512, 3, 256], P('walkers')
- log_amp_new: float32 [512], P('walkers')
- local_energy_new: float32 [512], P('walkers')
- energy_mean: float32 [], replicated
The draws below stay inside these ranges and needn't reach their ends.
Inputs may be any that keep to these rules, and one draw needn't show every extreme that they name: For every walker and spin, inverse is the inverse of the transpose of slater: the sum over o of slater[w, s, o, e] * inverse[w, s, o, f] is 1 when e = f and 0 otherwise, up to float32 rounding. `slater`: orbital values at the current positions. All counts sum to 512; for every whole m, the counts of the first m * 4 walkers sum to a value within 2 of m * 4, and both ends of that band are reached.
All inputs are finite; a program needn't handle non-finite values. No bound on the sum of `accepted` on one device may be relied on, other than what follows from the above.
Results may differ from the reference program's by a relative error of at most 0.0003.
Values sent between devices are 32-bit elements; how exact they have to be, the bound alone decides.
A program may use at most 64 MiB of HBM per device.

```python
import math
import jax
import jax.numpy as jnp
from jax import lax

NEL = 128
NB = 1024
K = 32
WINDOWS = 1
MOVES = 32
W_DEV = 4
WALKERS = 512


def slater_matrices(key):
    base = jax.random.fold_in(key, 7)
    shape = (WALKERS, 2, NEL, NEL)
    noise = jnp.clip(jax.random.normal(base, shape, jnp.float32), -4.0, 4.0)
    return 2.0 * jnp.eye(NEL, dtype=jnp.float32) + 0.5 * noise / math.sqrt(NEL)


def draw_slater(key, part):
    return slater_matrices(key)


def draw_inverse(key, part):
    return jnp.swapaxes(jnp.linalg.inv(slater_matrices(key)), 2, 3)


def draw_positions(key, part):
    walker_ids = jnp.arange(WALKERS).astype(jnp.float32)
    side = 4.0 * jnp.power(3.0, walker_ids / max(WALKERS - 1, 1))
    shape = (WALKERS, 3, 2 * NEL)
    cloud = jax.random.uniform(key, shape, jnp.float32, -0.5, 0.5)
    return 4.0 + side[:, None, None] * cloud


def draw_counts(key, part):
    devices = WALKERS // W_DEV
    half = W_DEV // 2
    keys = jax.random.split(key, 3)
    inner = jax.random.randint(keys[0], (devices - 1,), -half, half + 1)
    chosen = jax.random.randint(keys[1], (), 1, devices - 1)
    labels = jnp.arange(1, devices)
    inner = jnp.where(labels == chosen, -half, jnp.where(labels == chosen + 1, half, inner))
    edge = jnp.zeros((1,), jnp.int32)
    drift = jnp.concatenate([edge, inner.astype(jnp.int32), edge])
    totals = W_DEV + drift[1:] - drift[:-1]
    orders = jax.vmap(lambda piece: jax.random.permutation(piece, 2 * W_DEV))(jax.random.split(keys[2], devices))
    picked = (orders < totals[:, None]).astype(jnp.int32)
    return picked.reshape(devices, W_DEV, 2).sum(axis=2).reshape(WALKERS)


def touch_ends(drawn, rng, least, largest):
    spot = [jax.random.randint(jax.random.fold_in(rng, axis), (), 0, length) for axis, length in enumerate(drawn.shape)]
    widest = drawn.shape.index(max(drawn.shape))
    beside = spot[:widest] + [(spot[widest] + 1) % drawn.shape[widest]] + spot[widest + 1:]
    return drawn.at[tuple(spot)].set(least).at[tuple(beside)].set(largest)


def block_levels(key, shape, cuts, low, top_value):
    def one(axis_at, shards_of):
        steps = jax.random.uniform(jax.random.fold_in(jax.random.fold_in(key, 6), axis_at), (shards_of,), jnp.float32, low / len(cuts), top_value / len(cuts))
        return jnp.repeat(jnp.exp(steps), shape[axis_at] // shards_of).reshape((-1,) + (1,) * (len(shape) - axis_at - 1))

    loudness = one(*cuts[0])
    for cut in cuts[1:]:
        loudness = loudness * one(*cut)
    return loudness


def scatter_about(rng, shape, width, bound, cuts=(), kind=jnp.bfloat16):
    drawn = jax.random.normal(rng, shape, jnp.float32) * width
    if len(cuts) > 0:
        drawn = block_levels(rng, shape, cuts, -0.22, 0.18) * drawn
    return jnp.clip(drawn, min=-bound, max=bound).astype(kind)


def setup_inputs(seed: int = 0) -> dict:
    arg_keys = jax.random.split(jax.random.key(seed), 13)
    inverse = draw_inverse(jax.random.fold_in(arg_keys[12], 71), 0)
    slater = draw_slater(jax.random.fold_in(arg_keys[12], 71), 0)
    positions = draw_positions(jax.random.fold_in(arg_keys[12], 71), 0)
    displacements = scatter_about(arg_keys[3], (WALKERS, 3, 2 * NEL), 0.2, 0.6, ((0, 128),), jnp.float32)
    move_order = jax.vmap(lambda own: jax.random.permutation(own, NEL))(jax.random.split(arg_keys[4], WALKERS * 2)).reshape((WALKERS, 2, NEL)).astype(jnp.int32)
    accepted = touch_ends((jax.random.randint(arg_keys[5], (WALKERS, 2, MOVES), 0, 4) < 3).astype(jnp.int32), jax.random.fold_in(arg_keys[5], 1), 0, 1)
    counts = draw_counts(jax.random.fold_in(arg_keys[12], 71), 0)
    log_amp = scatter_about(arg_keys[7], (WALKERS,), 1.0, 4.0, ((0, 128),), jnp.float32)
    centers = jnp.clip(jax.random.uniform(arg_keys[8], (3, NB), jnp.float32, 0.0, 8.0), 0.0, 8.0)
    exponents = jnp.clip(jnp.exp(jax.random.uniform(arg_keys[9], (NB,), jnp.float32, math.log(0.3), math.log(3.0))), 0.3, 3.0)
    orbitals = scatter_about(arg_keys[10], (2, NEL, NB), 0.06, 0.36, ((1, 4),), jnp.float32)
    jastrow = jnp.clip(jax.random.uniform(arg_keys[11], (4,), jnp.float32, 0.2, 0.6), 0.2, 0.6)
    return dict(inverse=inverse, slater=slater, positions=positions, displacements=displacements, move_order=move_order, accepted=accepted, counts=counts, log_amp=log_amp, centers=centers, exponents=exponents, orbitals=orbitals, jastrow=jastrow)


highest = lax.Precision.HIGHEST

def basis_values(points, centers, exponents):
    squares = jnp.zeros((centers.shape[1], points.shape[1]), jnp.float32)
    for component in range(3):
        offset = points[component][None, :] - centers[component][:, None]
        squares = squares + offset * offset
    return jnp.exp(-exponents[:, None] * squares)

def orbital_change(points, steps, centers, exponents, orbitals):
    count = points.shape[1] // 2
    differ = basis_values(points + steps, centers, exponents) - basis_values(points, centers, exponents)
    spin_up = jnp.dot(orbitals[0].astype(jnp.float32), differ[:, :count].astype(jnp.float32), precision=highest, preferred_element_type=jnp.float32)
    spin_down = jnp.dot(orbitals[1].astype(jnp.float32), differ[:, count:].astype(jnp.float32), precision=highest, preferred_element_type=jnp.float32)
    return jnp.stack([spin_up, spin_down])

def pair_terms(before, after, jastrow):
    total = before.shape[1]
    old_squares = jnp.zeros((total, total), jnp.float32)
    new_squares = jnp.zeros((total, total), jnp.float32)
    for component in range(3):
        old_offset = before[component][:, None] - before[component][None, :]
        new_offset = after[component][:, None] - after[component][None, :]
        old_squares = old_squares + old_offset * old_offset
        new_squares = new_squares + new_offset * new_offset
    spins = jnp.arange(total) // (total // 2)
    same = spins[:, None] == spins[None, :]
    height = jnp.where(same, jastrow[0], jastrow[1])
    falloff = jnp.where(same, jastrow[2], jastrow[3])
    old_dist = jnp.sqrt(old_squares)
    new_dist = jnp.sqrt(new_squares)
    change = jnp.sum(height * (new_dist / (1.0 + falloff * new_dist) - old_dist / (1.0 + falloff * old_dist)))
    soft = jnp.sum(1.0 / jnp.sqrt(new_squares + 1.0))
    return (change, soft)

def eliminate(coupling, change):
    size = coupling.shape[-1]
    matrix = jnp.concatenate([coupling, change], axis=-1)
    labels = jnp.arange(size)

    def sweep(index, carry):
        matrix, logsum = carry
        pivot_row = lax.dynamic_slice_in_dim(matrix, index, 1, matrix.ndim - 2)
        pivot = lax.dynamic_slice_in_dim(pivot_row, index, 1, matrix.ndim - 1)
        pivot_row = pivot_row / pivot
        column_now = lax.dynamic_slice_in_dim(matrix, index, 1, matrix.ndim - 1)
        mine = (labels == index)[:, None]
        matrix = jnp.where(mine, pivot_row, matrix - column_now * pivot_row)
        return (matrix, logsum + jnp.log(jnp.abs(pivot[..., 0, 0])))
    start = (matrix, jnp.zeros(coupling.shape[:-2], jnp.float32))
    matrix, logsum = lax.fori_loop(0, size, sweep, start)
    return (matrix[..., size:], logsum)

def reference(inverse, slater, positions, displacements, move_order, accepted, counts, log_amp, centers, exponents, orbitals, jastrow):

    def per_walker(pair):
        return orbital_change(pair[0], pair[1], centers, exponents, orbitals)
    orbital_shift = lax.map(per_walker, (positions, displacements))
    proposed = slater + orbital_shift
    labels = jnp.arange(NEL)
    current = inverse
    logdet = jnp.zeros(inverse.shape[:2], jnp.float32)
    for window in range(WINDOWS):
        chosen = move_order[:, :, window * K:(window + 1) * K]
        flags = accepted[:, :, window * K:(window + 1) * K]
        one_hot = (labels[None, None, :, None] == chosen[:, :, None, :]).astype(jnp.float32)
        proposed_cols = jnp.einsum('wsoe,wsek->wsok', proposed, one_hot, precision=highest)
        intersection = jnp.einsum('wsok,wsoe->wske', proposed_cols, current, precision=highest)
        unit_rows = jnp.swapaxes(one_hot, 2, 3)
        effective = jnp.where(flags[..., None] == 1, intersection, unit_rows)
        coupling = jnp.einsum('wske,wsel->wskl', effective, one_hot, precision=highest)
        solved, logsum = eliminate(coupling, effective - unit_rows)
        columns = jnp.einsum('wsoe,wsek->wsok', current, one_hot, precision=highest)
        current = current - jnp.einsum('wsok,wske->wsoe', columns, solved, precision=highest)
        logdet = logdet + logsum
    placed = (move_order[:, :, :MOVES, None] == labels[None, None, None, :]).astype(jnp.float32)
    applied = jnp.einsum('wsk,wske->wse', accepted.astype(jnp.float32), placed, precision=highest)
    slater_now = slater + orbital_shift * applied[:, :, None, :]
    positions_now = positions + displacements * applied.reshape(applied.shape[0], 1, 2 * NEL)

    def walker_pairs(pair):
        return pair_terms(pair[0], pair[1], jastrow)
    jastrow_change, soft_total = lax.map(walker_pairs, (positions, positions_now))
    log_now = log_amp + lax.optimization_barrier(jnp.sum(logdet, axis=1)) + 0.5 * jastrow_change
    energy = (soft_total - 2.0 * NEL) / (2.0 * NEL * (2 * NEL - 1))
    energy_mean = jnp.sum(counts.astype(jnp.float32) * energy) / WALKERS
    limits = jnp.cumsum(counts).astype(jnp.int32)
    slot_ids = jnp.arange(WALKERS).astype(jnp.int32)
    source = lax.optimization_barrier(jnp.sum((limits[None, :] <= slot_ids[:, None]).astype(jnp.int32), axis=1))
    inverse_new = jnp.take(current, source, axis=0)
    slater_new = jnp.take(slater_now, source, axis=0)
    positions_new = jnp.take(positions_now, source, axis=0)
    log_amp_new = jnp.take(log_now, source, axis=0)
    local_energy_new = jnp.take(energy, source, axis=0)
    return (inverse_new, slater_new, positions_new, log_amp_new, local_energy_new, energy_mean)
```

```python
import math

import jax
import jax.numpy as jnp
from jax import lax
from jax.experimental import pallas as pl
from jax.experimental.pallas import tpu as pltpu
from jax.sharding import PartitionSpec as P

NEL = 128
K = 32
WD = 4
F32 = jnp.float32
BF16 = jnp.bfloat16
MESH = pl.DeviceIdType.MESH
LOG2E = math.log2(math.e)


def split(x):
    high = x.astype(BF16)
    return high, (x - high.astype(F32)).astype(BF16)


def product(a, b, dims):
    return lax.dot_general(a, b, (dims, ((), ())), preferred_element_type=F32)


NN = ((1,), (0,))
NT = ((1,), (1,))
TN = ((0,), (0,))


def product3(a, b, dims=NN):
    ah, al = a
    bh, bl = b
    return product(ah, bh, dims) + product(ah, bl, dims) + product(al, bh, dims)


def iota(shape, dim):
    return lax.broadcasted_iota(jnp.int32, shape, dim)


def flag(cond):
    return jnp.full((8, 128), cond.astype(jnp.int32), jnp.int32) == 1


def splat(x):
    return jnp.broadcast_to(x, (8, 128))


def pick(mask, new, old):
    rows = new.shape[0]
    new3, old3 = new.reshape(rows // 8, 8, 128), old.reshape(rows // 8, 8, 128)
    return jnp.where(mask[None], new3, old3).reshape(rows, 128)


def kernel(
    planes,
    plane,
    counts,
    jastrow,
    log_amp,
    inv_hbm,
    sla_hbm,
    pos_hbm,
    dis_hbm,
    mo_hbm,
    acc_hbm,
    cen_hbm,
    ex_hbm,
    orb_hbm,
    out_inv,
    out_sla,
    out_pos,
    out_log,
    out_en,
    out_mean,
    inv,
    sla,
    pos,
    dis,
    mo,
    acc,
    cen,
    ex,
    orb,
    dhi,
    dlo,
    oh,
    oha,
    ac,
    misc,
    here,
    logt,
    snd_a,
    part,
    rcv_a,
    rcv_b,
    solv,
    sla_r,
    sla_l,
    rs_r,
    rs_l,
    inv_r,
    inv_l,
    ri_r,
    ri_l,
    row_a,
    row_b,
    tab_a,
    tab_b,
    in_sem,
    send_x,
    recv_x,
    send_a,
    recv_a,
    send_b,
    recv_b,
):
    me = lax.axis_index("walkers")
    ob = lax.axis_index("orb")
    walkers = planes * plane
    core = ob % 2
    partner = (ob // 2) * 2 + (1 - core)
    across = (1 - ob // 2) * 2 + core
    right = (me + 1) % walkers
    left = (me + walkers - 1) % walkers
    z, r = me // plane, me % plane

    def at(w, o):
        return {"walkers": w, "orb": o}

    barrier = pltpu.get_barrier_semaphore()

    def greet(w, o):
        pl.semaphore_signal(barrier, inc=1, device_id=at(w, o), device_id_type=MESH)

    greet(me, partner)
    greet(me, across)
    greet(right, ob)
    greet(left, ob)

    @pl.loop(1, plane)
    def _(t):
        greet(z * plane + (r + t) % plane, ob)

    @pl.loop(1, planes)
    def _(t):
        greet(((z + t) % planes) * plane + r, ob)

    loads = [
        pltpu.make_async_copy(src, dst, in_sem.at[n])
        for n, (src, dst) in enumerate(
            (
                (mo_hbm, mo),
                (acc_hbm, acc),
                (pos_hbm, pos),
                (dis_hbm, dis),
                (cen_hbm, cen),
                (ex_hbm, ex),
                (orb_hbm, orb),
                (inv_hbm, inv),
                (sla_hbm, sla),
            )
        )
    ]
    for load in loads:
        load.start()
    for load in loads[:6]:
        load.wait()

    for w in range(WD):
        for c in range(3):
            for s in range(2):
                cols = slice(s * NEL, (s + 1) * NEL)
                n = 2 * c + s
                here[w, n : n + 1, :] = pos[c, w : w + 1, cols]
                here[w, n + 8 : n + 9, :] = dis[c, w : w + 1, cols]

    lane = iota((K, 128), 1)
    diag = lane == iota((K, 128), 0)

    @pl.loop(0, 2 * WD)
    def _(b):
        w, s = b // 2, b % 2
        order = mo[pl.ds(b, 1), :].astype(F32)
        taken = acc[pl.ds(b, 1), :].astype(F32)
        ek = jnp.sum(jnp.where(diag, order, 0.0), axis=1, keepdims=True)
        ak = jnp.sum(
            jnp.where(diag[:, :K], taken, 0.0), axis=1, keepdims=True
        )
        one = jnp.where(lane.astype(F32) == ek, 1.0, 0.0)
        took = one * ak
        rows = pl.ds(pl.multiple_of(b * K, K), K)
        oh[rows, :] = one.astype(BF16)
        oha[rows, :] = took.astype(BF16)
        ac[rows, :] = jnp.broadcast_to(ak, (K, 128))
        applied = jnp.sum(took, axis=0, keepdims=True)
        old, new = [], []
        for c in range(3):
            p = here[w, pl.ds(2 * c + s, 1), :]
            d = here[w, pl.ds(2 * c + s + 8, 1), :]
            old.append(jnp.sum(one * p, axis=1, keepdims=True))
            new.append(jnp.sum(one * (p + d), axis=1, keepdims=True))
            misc[w, pl.ds(2 * c + s, 1), :] = p + d * applied
        old = [jnp.broadcast_to(v, (K, 128)) for v in old]
        new = [jnp.broadcast_to(v, (K, 128)) for v in new]
        to = pl.ds(pl.multiple_of(w * K, K), K)
        for n in range(8):
            span = slice(n * 128, (n + 1) * 128)
            rate = ex[n : n + 1, :] * (-LOG2E)
            far = jnp.zeros((K, 128), F32)
            near = jnp.zeros((K, 128), F32)
            for c in range(3):
                center = cen[c : c + 1, span]
                a, e = old[c] - center, new[c] - center
                far = far + a * a
                near = near + e * e
            differ = jnp.exp2(rate * near) - jnp.exp2(rate * far)
            high, low = split(differ)
            dhi[s, to, span] = high
            dlo[s, to, span] = low

    loads[6].wait()
    shift = []
    for s in range(2):
        high, low = split(orb[s])
        high4 = jnp.concatenate([high] * 4, axis=0)
        low4 = jnp.concatenate([low] * 4, axis=0)
        a = dhi[s]
        shift.append(product(a, high4, NT) + product(a, low4, NT) + product(dlo[s], high4, NT))

    seg = iota((K, 128), 1) // K

    def block_rows(parts):
        return jnp.concatenate(
            [jnp.where(seg == n, x, 0.0) for n, x in enumerate(parts)], axis=0
        )

    shift_blocks = []
    for g in range(2):
        shift_blocks.append(
            split(
                block_rows(
                    [
                        shift[b % 2][(2 * g + b // 2) * K : (2 * g + b // 2 + 1) * K]
                        for b in range(4)
                    ]
                )
            )
        )

    loads[7].wait()
    change = []
    for g in range(2):
        rows = slice(g * 128, (g + 1) * 128)
        full = product3(shift_blocks[g], split(inv[rows, :]))
        change.append(jnp.where(ac[rows, :] > 0.5, full, 0.0))
    first = core == 0
    mine_mask = flag(first)
    snd_a[...] = pick(mine_mask, change[1], change[0])
    part[...] = pick(mine_mask, change[0], change[1])

    pl.semaphore_wait(barrier, 4 + (plane - 1) + (planes - 1))

    def remote(src, dst, n, w, o):
        return pltpu.make_async_remote_copy(
            src_ref=src,
            dst_ref=dst,
            send_sem=send_x.at[n],
            recv_sem=recv_x.at[n],
            device_id=at(w, o),
            device_id_type=MESH,
        )

    to_partner = remote(snd_a, rcv_a, 0, me, partner)
    to_partner.start()

    loads[8].wait()
    sla_now = []
    for g in range(2):
        rows = slice(g * 128, (g + 1) * 128)
        high, low = shift_blocks[g]
        taken = oha[rows, :]
        added = product(high, taken, TN) + product(low, taken, TN)
        sla[rows, :] = sla[rows, :] + added

    to_partner.wait_recv()
    part[...] = part[...] + rcv_a[...]
    to_across = remote(part, rcv_b, 1, me, across)
    to_across.start()

    c = [counts[n] for n in range(WD)]
    limit = [c[0]]
    for n in range(1, WD):
        limit.append(limit[-1] + c[n])
    start = [limit[n] - c[n] for n in range(WD)]
    total = limit[-1]

    def copy_masks(j):
        return [flag((start[n] <= j) & (j < limit[n])) for n in range(WD)]

    right_masks = [copy_masks(total - 1), copy_masks(total - 2)]
    left_masks = [copy_masks(jnp.int32(0)), copy_masks(jnp.int32(1))]

    def chosen(masks, parts):
        out = jnp.zeros_like(parts[0])
        for m, x in zip(masks, parts):
            out = pick(m, x, out)
        return out

    sub32 = iota((32, 128), 0)
    lane32 = iota((32, 128), 1)

    @pl.loop(0, WD)
    def _(w):
        ja = jnp.zeros((32, 128), F32)
        sa = jnp.zeros((32, 128), F32)
        for si, sj, weight in ((0, 0, 1.0), (1, 1, 1.0), (0, 1, 2.0)):
            height = jastrow[0 if si == sj else 1]
            falloff = jastrow[2 if si == sj else 3]

            def chunk(n, carry):
                ja, sa = carry
                on = lane32 == sub32 + 32 * n
                old_sq = jnp.zeros((32, 128), F32)
                new_sq = jnp.zeros((32, 128), F32)
                for c in range(3):
                    oi = here[w, 2 * c + si : 2 * c + si + 1, :]
                    oj = here[w, 2 * c + sj : 2 * c + sj + 1, :]
                    ni = misc[w, 2 * c + si : 2 * c + si + 1, :]
                    nj = misc[w, 2 * c + sj : 2 * c + sj + 1, :]
                    oc = jnp.sum(jnp.where(on, oi, 0.0), axis=1, keepdims=True)
                    nc = jnp.sum(jnp.where(on, ni, 0.0), axis=1, keepdims=True)
                    a, e = oc - oj, nc - nj
                    old_sq = old_sq + a * a
                    new_sq = new_sq + e * e
                od, nd = jnp.sqrt(old_sq), jnp.sqrt(new_sq)
                term = nd / (1.0 + falloff * nd) - od / (1.0 + falloff * od)
                soft = 1.0 / jnp.sqrt(new_sq + 1.0)
                return ja + (height * weight) * term, sa + weight * soft

            ja, sa = lax.fori_loop(0, 4, chunk, (ja, sa))
        jt = jnp.sum(jnp.sum(ja, axis=0, keepdims=True), axis=1, keepdims=True)
        st = jnp.sum(jnp.sum(sa, axis=0, keepdims=True), axis=1, keepdims=True)
        energy = (st - 2.0 * NEL) / (2.0 * NEL * (2 * NEL - 1))
        misc[w, 6:7, :] = jnp.broadcast_to(energy, (1, 128))
        misc[w, 7:8, :] = jnp.broadcast_to(jt, (1, 128))

    def pack(dst, masks, parts, n_rows):
        for n in range(2):
            dst[n * n_rows : (n + 1) * n_rows, :] = chosen(masks[n], parts)

    tiles = [misc[n] for n in range(WD)]
    slaters = [sla[n * 64 : (n + 1) * 64, :] for n in range(WD)]
    pack(sla_r, right_masks, slaters, 64)
    pack(sla_l, left_masks, slaters, 64)
    for n in range(2):
        sla_r[128 + 8 * n : 136 + 8 * n, :] = chosen(right_masks[n], tiles)
        sla_l[128 + 8 * n : 136 + 8 * n, :] = chosen(left_masks[n], tiles)
    slater_right = remote(sla_r, rs_l, 3, right, ob)
    slater_left = remote(sla_l, rs_r, 4, left, ob)
    slater_right.start()
    slater_left.start()

    l1 = iota((1, 128), 1)
    weighted = jnp.zeros((1, 128), F32)
    for n in range(WD):
        weighted = weighted + c[n].astype(F32) * tiles[n][6:7, :]
    own = jnp.where(l1 == 0, total.astype(F32), jnp.where(l1 == 1, weighted, 0.0))
    row_a[...] = own

    def in_plane(q):
        return pltpu.make_async_remote_copy(
            src_ref=row_a,
            dst_ref=tab_a.at[r],
            send_sem=send_a.at[q],
            recv_sem=recv_a.at[r],
            device_id=at(z * plane + q, ob),
            device_id_type=MESH,
        )

    def from_plane(q):
        return pltpu.make_async_remote_copy(
            src_ref=row_a,
            dst_ref=tab_a.at[q],
            send_sem=send_a.at[q],
            recv_sem=recv_a.at[q],
            device_id=at(z * plane + q, ob),
            device_id_type=MESH,
        )

    @pl.loop(1, plane)
    def _(t):
        in_plane((r + t) % plane).start()

    column_blocks = []
    block_on = (iota((128, 128), 0) // K) == (iota((128, 128), 1) // K)
    for g in range(2):
        rows = slice(g * 128, (g + 1) * 128)
        high, low = split(inv[rows, :])
        which = oh[rows, :]
        got = product(high, which, NT) + product(low, which, NT)
        column_blocks.append(split(jnp.where(block_on, got, 0.0)))

    to_across.wait_recv()
    summed = part[...] + rcv_b[...]
    high, low = split(summed)
    which = oh[pl.ds(pl.multiple_of(core * 128, 128), 128), :]
    got = product(high, which, NT) + product(low, which, NT)
    lane8 = iota((8, 128), 1)
    sub8 = iota((8, 128), 0)
    seg8 = lane8 // K
    in_seg = lane8 % K
    tile = []
    for t in range(4):
        x = jnp.where(in_seg == sub8 + 8 * t, 1.0, 0.0)
        for b in range(4):
            x = x + jnp.where(seg8 == b, got[b * K + 8 * t : b * K + 8 * t + 8], 0.0)
        tile.append(x)

    def panel(p, carry):
        m, logs = list(carry[:4]), carry[4]
        base = 8 * p
        cols = [
            [jnp.take_along_axis(m[t], seg8 * K + base + n, axis=1) for t in range(4)]
            for n in range(8)
        ]
        pivots = jnp.ones((8, 128), F32)
        for n in range(8):
            bk = cols[n]
            pivot = bk[0][n : n + 1, :]
            inverse_pivot = 1.0 / pivot
            pivots = jnp.where(sub8 == n, pivot, pivots)
            spot = in_seg == base + n
            row = jnp.where(spot, inverse_pivot, m[0][n : n + 1, :] * inverse_pivot)
            for t in range(4):
                fresh = jnp.where(spot, 0.0, m[t]) - bk[t] * row
                m[t] = jnp.where(sub8 == n, row, fresh) if t == 0 else fresh
            for j in range(n + 1, 8):
                scale = cols[j][0][n : n + 1, :] * inverse_pivot
                for t in range(4):
                    fresh = cols[j][t] - bk[t] * scale
                    cols[j][t] = jnp.where(sub8 == n, scale, fresh) if t == 0 else fresh
        logs = logs + jnp.log(jnp.abs(pivots))
        return m[1], m[2], m[3], m[0], logs

    *tile, logs = lax.fori_loop(0, 4, panel, (*tile, jnp.zeros((8, 128), F32)))
    reverse = jnp.concatenate(tile, axis=0)
    solved = product3(split(block_rows([reverse] * 4)), (high, low))
    logdet = jnp.broadcast_to(jnp.sum(logs, axis=0, keepdims=True), (8, 128))
    solv[core, 0:128, :] = solved
    solv[core, 128:136, :] = logdet
    swap = remote(solv.at[core], solv.at[core], 2, me, partner)
    swap.start()

    @pl.loop(1, plane)
    def _(t):
        from_plane((r + t) % plane).wait_recv()

    def table(tab, rows, place, own_row):
        before = jnp.zeros((1, 128), F32)
        every = jnp.zeros((1, 128), F32)
        for n in range(rows):
            x = jnp.where(jnp.full((1, 128), place, jnp.int32) == n, own_row, tab[n])
            before = before + jnp.where(jnp.full((1, 128), place, jnp.int32) > n, x, 0.0)
            every = every + x
        return before, every

    before_a, every_a = table(tab_a, plane, r, own)
    row_b[...] = every_a

    def in_column(q, slot):
        return pltpu.make_async_remote_copy(
            src_ref=row_b,
            dst_ref=tab_b.at[slot],
            send_sem=send_b.at[q],
            recv_sem=recv_b.at[slot],
            device_id=at(q * plane + r, ob),
            device_id_type=MESH,
        )

    @pl.loop(1, planes)
    def _(t):
        in_column((z + t) % planes, z).start()

    swap_in = remote(solv.at[1 - core], solv.at[1 - core], 2, me, partner)
    swap_in.wait_recv()
    for g in range(2):
        rows = slice(g * 128, (g + 1) * 128)
        inv[rows, :] = inv[rows, :] - product3(column_blocks[g], split(solv[g, 0:128, :]))
    for n in range(WD):
        row = solv[n // 2, 128:136, :]
        base = 64 * (n % 2)
        up_down = jnp.where((lane8 == base) | (lane8 == base + K), row, 0.0)
        both = splat(jnp.sum(up_down, axis=1, keepdims=True))
        logt[8 * n : 8 * n + 8, :] = (log_amp[n] + both) + 0.5 * splat(tiles[n][7:8, :])
    inverses = [inv[n * 64 : (n + 1) * 64, :] for n in range(WD)]
    log_tiles = [logt[8 * n : 8 * n + 8, :] for n in range(WD)]
    pack(inv_r, right_masks, inverses, 64)
    pack(inv_l, left_masks, inverses, 64)
    for n in range(2):
        inv_r[128 + 8 * n : 136 + 8 * n, :] = chosen(right_masks[n], log_tiles)
        inv_l[128 + 8 * n : 136 + 8 * n, :] = chosen(left_masks[n], log_tiles)
    inverse_right = remote(inv_r, ri_l, 5, right, ob)
    inverse_left = remote(inv_l, ri_r, 6, left, ob)
    inverse_right.start()
    inverse_left.start()

    @pl.loop(1, planes)
    def _(t):
        q = (z + t) % planes
        in_column(q, q).wait_recv()

    before_b, every_b = table(tab_b, planes, z, every_a)
    out_mean[0] = jnp.sum(jnp.where(l1 == 1, every_b, 0.0)) / (WD * walkers)
    ahead = jnp.where(l1 == 0, before_a + before_b, 0.0)
    over = splat(jnp.sum(ahead, axis=1, keepdims=True)) - (WD * me).astype(F32)

    slater_right.wait_recv()
    slater_left.wait_recv()
    inverse_right.wait_recv()
    inverse_left.wait_recv()

    totalf = total.astype(F32)
    for i in range(WD):
        j = i - over
        masks = [j == -1.0, j == -2.0]
        masks += [
            (j >= start[n].astype(F32)) & (j < limit[n].astype(F32)) for n in range(WD)
        ]
        masks += [j == totalf, j == totalf + 1.0]

        def halo(ref_l, ref_r, n_rows, base):
            return [ref_l[base + n * n_rows : base + (n + 1) * n_rows, :] for n in range(2)], [
                ref_r[base + n * n_rows : base + (n + 1) * n_rows, :] for n in range(2)
            ]

        def select(own_parts, ref_l, ref_r, n_rows, base):
            a, e = halo(ref_l, ref_r, n_rows, base)
            return chosen(masks, a + own_parts + e)

        out_inv[i * 64 : (i + 1) * 64, :] = select(
            [inv[n * 64 : (n + 1) * 64, :] for n in range(WD)], ri_l, ri_r, 64, 0
        )
        out_sla[i * 64 : (i + 1) * 64, :] = select(
            [sla[n * 64 : (n + 1) * 64, :] for n in range(WD)], rs_l, rs_r, 64, 0
        )
        small = select([misc[n] for n in range(WD)], rs_l, rs_r, 8, 128)
        logs_here = select(
            [logt[8 * n : 8 * n + 8, :] for n in range(WD)], ri_l, ri_r, 8, 128
        )
        for c3 in range(3):
            for s in range(2):
                out_pos[c3, i : i + 1, s * NEL : (s + 1) * NEL] = small[2 * c3 + s : 2 * c3 + s + 1]
        out_en[i] = small[6, 0]
        out_log[i] = logs_here[0, 0]

    for copy in (
        to_partner,
        to_across,
        swap,
        slater_right,
        slater_left,
        inverse_right,
        inverse_left,
    ):
        copy.wait_send()

    @pl.loop(1, plane)
    def _(t):
        in_plane((r + t) % plane).wait_send()

    @pl.loop(1, planes)
    def _(t):
        in_column((z + t) % planes, z).wait_send()


def solution(mesh):
    walkers = mesh.shape["walkers"]
    plane = 16 if walkers == 128 else walkers // 2
    planes = walkers // plane

    def body(
        inverse,
        slater,
        positions,
        displacements,
        move_order,
        accepted,
        counts,
        log_amp,
        centers,
        exponents,
        orbitals,
        jastrow,
    ):
        smem = pl.BlockSpec(memory_space=pltpu.SMEM)
        vmem = pl.BlockSpec(memory_space=pltpu.VMEM)
        hbm = pl.BlockSpec(memory_space=pl.ANY)

        def shape(*dims):
            return jax.ShapeDtypeStruct(dims, F32)

        def buf(*dims, kind=F32):
            return pltpu.VMEM(dims, kind)

        dma = pltpu.SemaphoreType.DMA
        outs = pl.pallas_call(
            lambda *refs: kernel(planes, plane, *refs),
            out_shape=(
                shape(256, 128),
                shape(256, 128),
                shape(3, 4, 256),
                shape(4),
                shape(4),
                shape(1),
            ),
            in_specs=[smem] * 3 + [hbm] * 9,
            out_specs=(vmem, vmem, vmem, smem, smem, smem),
            scratch_shapes=[
                buf(256, 128),
                buf(256, 128),
                buf(3, 4, 256),
                buf(3, 4, 256),
                buf(8, 128, kind=jnp.int32),
                buf(8, 32, kind=jnp.int32),
                buf(3, 1024),
                buf(8, 128),
                buf(2, 32, 1024),
                buf(2, 128, 1024, kind=BF16),
                buf(2, 128, 1024, kind=BF16),
                buf(256, 128, kind=BF16),
                buf(256, 128, kind=BF16),
                buf(256, 128),
                buf(4, 8, 128),
                buf(4, 16, 128),
                buf(32, 128),
                buf(128, 128),
                buf(128, 128),
                buf(128, 128),
                buf(128, 128),
                buf(2, 136, 128),
                *[buf(144, 128) for _ in range(8)],
                buf(1, 128),
                buf(1, 128),
                buf(plane, 1, 128),
                buf(planes, 1, 128),
                dma((9,)),
                dma((7,)),
                dma((7,)),
                dma((plane,)),
                dma((plane,)),
                dma((planes,)),
                dma((planes,)),
            ],
            compiler_params=pltpu.CompilerParams(collective_id=0, has_side_effects=True),
            name="generation",
        )(
            counts,
            jastrow,
            log_amp,
            inverse.reshape(256, 128),
            slater.reshape(256, 128),
            positions.transpose(1, 0, 2),
            displacements.transpose(1, 0, 2),
            move_order.reshape(8, 128),
            accepted.reshape(8, 32),
            centers,
            exponents.reshape(8, 128),
            orbitals,
        )
        return (
            outs[0].reshape(4, 2, 32, 128),
            outs[1].reshape(4, 2, 32, 128),
            outs[2].transpose(1, 0, 2),
            outs[3],
            outs[4],
            outs[5].reshape(()),
        )

    placed = (
        P("walkers", None, "orb", None),
        P("walkers", None, "orb", None),
        P("walkers", None, None),
        P("walkers", None, None),
        P("walkers", None, None),
        P("walkers", None, None),
        P("walkers"),
        P("walkers"),
        P(),
        P(),
        P(None, "orb", None),
        P(),
    )
    return jax.shard_map(
        body,
        mesh=mesh,
        in_specs=placed,
        out_specs=(
            P("walkers", None, "orb", None),
            P("walkers", None, "orb", None),
            P("walkers", None, None),
            P("walkers"),
            P("walkers"),
            P(),
        ),
        check_vma=False,
    )
```

```python
import math

import jax
import jax.numpy as jnp
from jax import lax
from jax.experimental import pallas as pl
from jax.experimental.pallas import tpu as pltpu
from jax.sharding import PartitionSpec as P

NEL = 128
K = 32
WD = 4
F32 = jnp.float32
BF16 = jnp.bfloat16
MESH = pl.DeviceIdType.MESH
LOG2E = math.log2(math.e)


def split(x):
    high = x.astype(BF16)
    return high, (x - high.astype(F32)).astype(BF16)


def product(a, b, dims):
    return lax.dot_general(a, b, (dims, ((), ())), preferred_element_type=F32)


NN = ((1,), (0,))
NT = ((1,), (1,))
TN = ((0,), (0,))


def product3(a, b, dims=NN):
    ah, al = a
    bh, bl = b
    return product(ah, bh, dims) + product(ah, bl, dims) + product(al, bh, dims)


def iota(shape, dim):
    return lax.broadcasted_iota(jnp.int32, shape, dim)


def flag(cond):
    return jnp.full((8, 128), cond.astype(jnp.int32), jnp.int32) == 1


def splat(x):
    return jnp.broadcast_to(x, (8, 128))


def pick(mask, new, old):
    rows = new.shape[0]
    new3, old3 = new.reshape(rows // 8, 8, 128), old.reshape(rows // 8, 8, 128)
    return jnp.where(mask[None], new3, old3).reshape(rows, 128)


def kernel(
    planes,
    plane,
    cnt_hbm,
    jas_hbm,
    amp_hbm,
    inv_hbm,
    sla_hbm,
    pos_hbm,
    dis_hbm,
    mo_hbm,
    acc_hbm,
    cen_hbm,
    ex_hbm,
    orb_hbm,
    out,
    counts,
    jastrow,
    log_amp,
    inv,
    sla,
    pos,
    dis,
    mo,
    acc,
    cen,
    ex,
    orb,
    dhi,
    dlo,
    oh,
    oha,
    ac,
    misc,
    here,
    pts,
    logt,
    snd_a,
    part,
    rcv_a,
    rcv_b,
    solv,
    sla_r,
    sla_l,
    rs_r,
    rs_l,
    inv_r,
    inv_l,
    ri_r,
    ri_l,
    row_a,
    row_b,
    tab_a,
    tab_b,
    in_sem,
    send_x,
    recv_x,
    send_a,
    recv_a,
    send_b,
    recv_b,
):
    me = lax.axis_index("walkers")
    ob = lax.axis_index("orb")
    walkers = planes * plane
    core = ob % 2
    partner = (ob // 2) * 2 + (1 - core)
    across = (1 - ob // 2) * 2 + core
    z, r = me // plane, me % plane

    def at(w, o):
        return {"walkers": w, "orb": o}

    loads = [
        pltpu.make_async_copy(src, dst, in_sem.at[n])
        for n, (src, dst) in enumerate(
            (
                (mo_hbm, mo),
                (acc_hbm, acc),
                (pos_hbm, pos),
                (dis_hbm, dis),
                (cen_hbm, cen),
                (ex_hbm, ex),
                (orb_hbm, orb),
                (inv_hbm, inv),
                (sla_hbm, sla),
                (cnt_hbm, counts),
                (jas_hbm, jastrow),
                (amp_hbm, log_amp),
            )
        )
    ]
    for load in loads:
        load.start()
    barrier = pltpu.get_barrier_semaphore()

    def greet(w, o):
        pl.semaphore_signal(barrier, inc=1, device_id=at(w, o), device_id_type=MESH)

    greet(me, partner)
    greet(me, across)
    has_right, has_left = me < walkers - 1, me > 0

    @pl.when(has_right)
    def _():
        greet(me + 1, ob)

    @pl.when(has_left)
    def _():
        greet(me - 1, ob)

    @pl.when(me == 0)
    def _():
        rs_l[...] = jnp.zeros_like(rs_l)
        ri_l[...] = jnp.zeros_like(ri_l)

    @pl.when(me == walkers - 1)
    def _():
        rs_r[...] = jnp.zeros_like(rs_r)
        ri_r[...] = jnp.zeros_like(ri_r)

    @pl.loop(1, plane)
    def _(t):
        greet(z * plane + (r + t) % plane, ob)

    @pl.loop(1, planes)
    def _(t):
        greet(((z + t) % planes) * plane + r, ob)

    for load in loads[:6]:
        load.wait()

    for w in range(WD):
        for c in range(3):
            for s in range(2):
                cols = slice(s * NEL, (s + 1) * NEL)
                n = 2 * c + s
                here[w, n : n + 1, :] = pos[c, w : w + 1, cols]
                here[w, n + 8 : n + 9, :] = dis[c, w : w + 1, cols]

    lane = iota((K, 128), 1)
    diag = lane == iota((K, 128), 0)

    @pl.loop(0, 2 * WD)
    def _(b):
        w, s = b // 2, b % 2
        order = mo[pl.ds(b, 1), :].astype(F32)
        taken = acc[pl.ds(b, 1), :].astype(F32)
        ek = jnp.sum(jnp.where(diag, order, 0.0), axis=1, keepdims=True)
        ak = jnp.sum(
            jnp.where(diag[:, :K], taken, 0.0), axis=1, keepdims=True
        )
        one = jnp.where(lane.astype(F32) == ek, 1.0, 0.0)
        took = one * ak
        rows = pl.ds(pl.multiple_of(b * K, K), K)
        oh[rows, :] = one.astype(BF16)
        oha[rows, :] = took.astype(BF16)
        ac[rows, :] = jnp.broadcast_to(ak, (K, 128))
        applied = jnp.sum(took, axis=0, keepdims=True)
        old, new = [], []
        for c in range(3):
            p = here[w, pl.ds(2 * c + s, 1), :]
            d = here[w, pl.ds(2 * c + s + 8, 1), :]
            old.append(jnp.sum(one * p, axis=1, keepdims=True))
            new.append(jnp.sum(one * (p + d), axis=1, keepdims=True))
            misc[w, pl.ds(2 * c + s, 1), :] = p + d * applied
        for c in range(3):
            pts[c, rows, :] = jnp.broadcast_to(old[c], (K, 128))
            pts[c + 3, rows, :] = jnp.broadcast_to(new[c], (K, 128))

    for load in loads[9:]:
        load.wait()
    sub32 = iota((32, 128), 0)

    @pl.loop(0, WD)
    def _(w):
        zero = jnp.zeros((32, 128), F32)
        js, jd, es, ed = zero, zero, zero, zero

        def pair_block(oc, nc, sj, falloff, ja, ea):
            old_sq, new_sq = zero, zero
            for c in range(3):
                a = oc[c] - here[w, 2 * c + sj : 2 * c + sj + 1, :]
                e = nc[c] - misc[w, 2 * c + sj : 2 * c + sj + 1, :]
                old_sq = old_sq + a * a
                new_sq = new_sq + e * e
            od, nd = jnp.sqrt(old_sq), jnp.sqrt(new_sq)
            term = (nd - od) / ((1.0 + falloff * nd) * (1.0 + falloff * od))
            return ja + term, ea + lax.rsqrt(new_sq + 1.0)

        for si in range(2):
            for n in range(4):
                on = lane == sub32 + 32 * n
                oc, nc = [], []
                for c in range(3):
                    oi = here[w, 2 * c + si : 2 * c + si + 1, :]
                    ni = misc[w, 2 * c + si : 2 * c + si + 1, :]
                    oc.append(jnp.sum(jnp.where(on, oi, 0.0), axis=1, keepdims=True))
                    nc.append(jnp.sum(jnp.where(on, ni, 0.0), axis=1, keepdims=True))
                js, es = pair_block(oc, nc, si, jastrow[2], js, es)
                if si == 0:
                    jd, ed = pair_block(oc, nc, 1, jastrow[3], jd, ed)
        ja = jastrow[0] * js + (2.0 * jastrow[1]) * jd
        ea = es + 2.0 * ed
        jt = jnp.sum(jnp.sum(ja, axis=0, keepdims=True), axis=1, keepdims=True)
        st = jnp.sum(jnp.sum(ea, axis=0, keepdims=True), axis=1, keepdims=True)
        energy = (st - 2.0 * NEL) / (2.0 * NEL * (2 * NEL - 1))
        misc[w, 6:7, :] = jnp.broadcast_to(energy, (1, 128))
        misc[w, 7:8, :] = jnp.broadcast_to(jt, (1, 128))

    l1 = iota((1, 128), 1)
    c = [counts[n] for n in range(WD)]
    limit = [c[0]]
    for n in range(1, WD):
        limit.append(limit[-1] + c[n])
    start = [limit[n] - c[n] for n in range(WD)]
    total = limit[-1]
    tiles = [misc[n] for n in range(WD)]
    weighted = jnp.zeros((1, 128), F32)
    for n in range(WD):
        weighted = weighted + c[n].astype(F32) * tiles[n][6:7, :]
    own = jnp.where(l1 == 0, total.astype(F32), jnp.where(l1 == 1, weighted, 0.0))
    row_a[...] = own

    @pl.loop(0, 2 * WD)
    def _(b):
        w, s = b // 2, b % 2
        rows = pl.ds(pl.multiple_of(b * K, K), K)
        old = [pts[c, rows, :] for c in range(3)]
        new = [pts[c + 3, rows, :] for c in range(3)]
        to = pl.ds(pl.multiple_of(w * K, K), K)
        for n in range(8):
            span = slice(n * 128, (n + 1) * 128)
            rate = ex[n : n + 1, :] * (-LOG2E)
            far = jnp.zeros((K, 128), F32)
            near = jnp.zeros((K, 128), F32)
            for c in range(3):
                center = cen[c : c + 1, span]
                a, e = old[c] - center, new[c] - center
                far = far + a * a
                near = near + e * e
            differ = jnp.exp2(rate * near) - jnp.exp2(rate * far)
            high, low = split(differ)
            dhi[s, to, span] = high
            dlo[s, to, span] = low

    loads[6].wait()
    shift = []
    for s in range(2):
        high, low = split(orb[s])
        high4 = jnp.concatenate([high] * 4, axis=0)
        low4 = jnp.concatenate([low] * 4, axis=0)
        a = dhi[s]
        shift.append(product(a, high4, NT) + product(a, low4, NT) + product(dlo[s], high4, NT))

    seg = iota((K, 128), 1) // K

    def block_rows(parts):
        return jnp.concatenate(
            [jnp.where(seg == n, x, 0.0) for n, x in enumerate(parts)], axis=0
        )

    shift_blocks = []
    for g in range(2):
        shift_blocks.append(
            split(
                block_rows(
                    [
                        shift[b % 2][(2 * g + b // 2) * K : (2 * g + b // 2 + 1) * K]
                        for b in range(4)
                    ]
                )
            )
        )

    loads[7].wait()
    change = []
    for g in range(2):
        rows = slice(g * 128, (g + 1) * 128)
        full = product3(shift_blocks[g], split(inv[rows, :]))
        change.append(jnp.where(ac[rows, :] > 0.5, full, 0.0))
    first = core == 0
    mine_mask = flag(first)
    snd_a[...] = pick(mine_mask, change[1], change[0])
    part[...] = pick(mine_mask, change[0], change[1])

    neighbours = jnp.where(has_right, 1, 0) + jnp.where(has_left, 1, 0)
    pl.semaphore_wait(barrier, 2 + (plane - 1) + (planes - 1) + neighbours)

    def remote(src, dst, n, w, o):
        return pltpu.make_async_remote_copy(
            src_ref=src,
            dst_ref=dst,
            send_sem=send_x.at[n],
            recv_sem=recv_x.at[n],
            device_id=at(w, o),
            device_id_type=MESH,
        )

    to_partner = remote(snd_a, rcv_a, 0, me, partner)
    to_partner.start()

    def in_plane(q):
        return pltpu.make_async_remote_copy(
            src_ref=row_a,
            dst_ref=tab_a.at[r],
            send_sem=send_a.at[q],
            recv_sem=recv_a.at[r],
            device_id=at(z * plane + q, ob),
            device_id_type=MESH,
        )

    def from_plane(q):
        return pltpu.make_async_remote_copy(
            src_ref=row_a,
            dst_ref=tab_a.at[q],
            send_sem=send_a.at[q],
            recv_sem=recv_a.at[q],
            device_id=at(z * plane + q, ob),
            device_id_type=MESH,
        )

    @pl.loop(1, plane)
    def _(t):
        in_plane((r + t) % plane).start()


    loads[8].wait()
    sla_now = []
    for g in range(2):
        rows = slice(g * 128, (g + 1) * 128)
        high, low = shift_blocks[g]
        taken = oha[rows, :]
        added = product(high, taken, TN) + product(low, taken, TN)
        sla[rows, :] = sla[rows, :] + added

    to_partner.wait_recv()
    part[...] = part[...] + rcv_a[...]
    to_across = remote(part, rcv_b, 1, me, across)
    to_across.start()

    def copy_masks(j):
        return [flag((start[n] <= j) & (j < limit[n])) for n in range(WD)]

    right_masks = [copy_masks(total - 1), copy_masks(total - 2)]
    left_masks = [copy_masks(jnp.int32(0)), copy_masks(jnp.int32(1))]

    def chosen(masks, parts):
        out = jnp.zeros_like(parts[0])
        for m, x in zip(masks, parts):
            out = pick(m, x, out)
        return out

    def pack(dst, masks, parts, n_rows):
        for n in range(2):
            dst[n * n_rows : (n + 1) * n_rows, :] = chosen(masks[n], parts)

    slaters = [sla[n * 64 : (n + 1) * 64, :] for n in range(WD)]
    pack(sla_r, right_masks, slaters, 64)
    pack(sla_l, left_masks, slaters, 64)
    for n in range(2):
        sla_r[128 + 8 * n : 136 + 8 * n, :] = chosen(right_masks[n], tiles)
        sla_l[128 + 8 * n : 136 + 8 * n, :] = chosen(left_masks[n], tiles)

    column_blocks = []
    block_on = (iota((128, 128), 0) // K) == (iota((128, 128), 1) // K)
    for g in range(2):
        rows = slice(g * 128, (g + 1) * 128)
        high, low = split(inv[rows, :])
        which = oh[rows, :]
        got = product(high, which, NT) + product(low, which, NT)
        column_blocks.append(split(jnp.where(block_on, got, 0.0)))

    slater_right = remote(sla_r, rs_l, 3, me + 1, ob)
    slater_left = remote(sla_l, rs_r, 4, me - 1, ob)

    def start_both(to_right, to_left):
        @pl.when(has_right)
        def _():
            to_right.start()

        @pl.when(has_left)
        def _():
            to_left.start()

    to_across.wait_recv()
    start_both(slater_right, slater_left)
    summed = part[...] + rcv_b[...]
    high, low = split(summed)
    which = oh[pl.ds(pl.multiple_of(core * 128, 128), 128), :]
    got = product(high, which, NT) + product(low, which, NT)
    lane8 = iota((8, 128), 1)
    sub8 = iota((8, 128), 0)
    seg8 = lane8 // K
    in_seg = lane8 % K
    tile = []
    for t in range(4):
        x = jnp.where(in_seg == sub8 + 8 * t, 1.0, 0.0)
        for b in range(4):
            x = x + jnp.where(seg8 == b, got[b * K + 8 * t : b * K + 8 * t + 8], 0.0)
        tile.append(x)

    def panel(p, carry):
        m, logs = list(carry[:4]), carry[4]
        base = 8 * p
        cols = [
            [jnp.take_along_axis(m[t], seg8 * K + base + n, axis=1) for t in range(4)]
            for n in range(8)
        ]
        pivots = jnp.ones((8, 128), F32)
        for n in range(8):
            bk = cols[n]
            pivot = bk[0][n : n + 1, :]
            inverse_pivot = 1.0 / pivot
            pivots = jnp.where(sub8 == n, pivot, pivots)
            spot = in_seg == base + n
            row = jnp.where(spot, inverse_pivot, m[0][n : n + 1, :] * inverse_pivot)
            for t in range(4):
                fresh = jnp.where(spot, 0.0, m[t]) - bk[t] * row
                m[t] = jnp.where(sub8 == n, row, fresh) if t == 0 else fresh
            for j in range(n + 1, 8):
                scale = cols[j][0][n : n + 1, :] * inverse_pivot
                for t in range(4):
                    fresh = cols[j][t] - bk[t] * scale
                    cols[j][t] = jnp.where(sub8 == n, scale, fresh) if t == 0 else fresh
        logs = logs + jnp.log(jnp.abs(pivots))
        return m[1], m[2], m[3], m[0], logs

    *tile, logs = lax.fori_loop(0, 4, panel, (*tile, jnp.zeros((8, 128), F32)))
    reverse = jnp.concatenate(tile, axis=0)
    solved = product3(split(block_rows([reverse] * 4)), (high, low))
    logdet = jnp.broadcast_to(jnp.sum(logs, axis=0, keepdims=True), (8, 128))
    solv[core, 0:128, :] = solved
    solv[core, 128:136, :] = logdet
    swap = remote(solv.at[core], solv.at[core], 2, me, partner)
    swap.start()

    swap_in = remote(solv.at[1 - core], solv.at[1 - core], 2, me, partner)
    swap_in.wait_recv()
    for g in range(2):
        rows = slice(g * 128, (g + 1) * 128)
        inv[rows, :] = inv[rows, :] - product3(column_blocks[g], split(solv[g, 0:128, :]))
    for n in range(WD):
        row = solv[n // 2, 128:136, :]
        base = 64 * (n % 2)
        up_down = jnp.where((lane8 == base) | (lane8 == base + K), row, 0.0)
        both = splat(jnp.sum(up_down, axis=1, keepdims=True))
        logt[8 * n : 8 * n + 8, :] = (log_amp[n] + both) + 0.5 * splat(tiles[n][7:8, :])
    inverses = [inv[n * 64 : (n + 1) * 64, :] for n in range(WD)]
    log_tiles = [logt[8 * n : 8 * n + 8, :] for n in range(WD)]
    pack(inv_r, right_masks, inverses, 64)
    pack(inv_l, left_masks, inverses, 64)
    for n in range(2):
        inv_r[128 + 8 * n : 136 + 8 * n, :] = chosen(right_masks[n], log_tiles)
        inv_l[128 + 8 * n : 136 + 8 * n, :] = chosen(left_masks[n], log_tiles)
    inverse_right = remote(inv_r, ri_l, 5, me + 1, ob)
    inverse_left = remote(inv_l, ri_r, 6, me - 1, ob)
    start_both(inverse_right, inverse_left)

    @pl.loop(1, plane)
    def _(t):
        from_plane((r + t) % plane).wait_recv()

    def table(tab, rows, place, own_row):
        before = jnp.zeros((1, 128), F32)
        every = jnp.zeros((1, 128), F32)
        for n in range(rows):
            x = jnp.where(jnp.full((1, 128), place, jnp.int32) == n, own_row, tab[n])
            before = before + jnp.where(jnp.full((1, 128), place, jnp.int32) > n, x, 0.0)
            every = every + x
        return before, every

    before_a, every_a = table(tab_a, plane, r, own)
    row_b[...] = every_a

    def in_column(q, slot):
        return pltpu.make_async_remote_copy(
            src_ref=row_b,
            dst_ref=tab_b.at[slot],
            send_sem=send_b.at[q],
            recv_sem=recv_b.at[slot],
            device_id=at(q * plane + r, ob),
            device_id_type=MESH,
        )

    @pl.loop(1, planes)
    def _(t):
        in_column((z + t) % planes, z).start()

    @pl.loop(1, planes)
    def _(t):
        q = (z + t) % planes
        in_column(q, q).wait_recv()

    before_b, every_b = table(tab_b, planes, z, every_a)
    mean = jnp.sum(jnp.where(l1 == 1, every_b, 0.0), axis=1, keepdims=True)
    out[552:560, :] = splat(mean) / (WD * walkers)
    ahead = jnp.where(l1 == 0, before_a + before_b, 0.0)
    over = splat(jnp.sum(ahead, axis=1, keepdims=True)) - (WD * me).astype(F32)

    @pl.when(has_left)
    def _():
        slater_right.wait_recv()
        inverse_right.wait_recv()

    @pl.when(has_right)
    def _():
        slater_left.wait_recv()
        inverse_left.wait_recv()

    totalf = total.astype(F32)
    for i in range(WD):
        j = i - over
        masks = [j == -1.0, j == -2.0]
        masks += [
            (j >= start[n].astype(F32)) & (j < limit[n].astype(F32)) for n in range(WD)
        ]
        masks += [j == totalf, j == totalf + 1.0]

        def halo(ref_l, ref_r, n_rows, base):
            return [ref_l[base + n * n_rows : base + (n + 1) * n_rows, :] for n in range(2)], [
                ref_r[base + n * n_rows : base + (n + 1) * n_rows, :] for n in range(2)
            ]

        def select(own_parts, ref_l, ref_r, n_rows, base):
            a, e = halo(ref_l, ref_r, n_rows, base)
            return chosen(masks, a + own_parts + e)

        out[i * 64 : (i + 1) * 64, :] = select(
            [inv[n * 64 : (n + 1) * 64, :] for n in range(WD)], ri_l, ri_r, 64, 0
        )
        out[256 + i * 64 : 256 + (i + 1) * 64, :] = select(
            [sla[n * 64 : (n + 1) * 64, :] for n in range(WD)], rs_l, rs_r, 64, 0
        )
        small = select([misc[n] for n in range(WD)], rs_l, rs_r, 8, 128)
        logs_here = select(
            [logt[8 * n : 8 * n + 8, :] for n in range(WD)], ri_l, ri_r, 8, 128
        )
        for n in range(6):
            row = 512 + 4 * n + i
            out[row : row + 1, :] = small[n : n + 1, :]
        out[536 + i : 537 + i, :] = logs_here[0:1, :]
        out[544 + i : 545 + i, :] = small[6:7, :]

    for copy in (
        to_partner,
        to_across,
        swap,
    ):
        copy.wait_send()

    @pl.when(has_right)
    def _():
        slater_right.wait_send()
        inverse_right.wait_send()

    @pl.when(has_left)
    def _():
        slater_left.wait_send()
        inverse_left.wait_send()

    @pl.loop(1, plane)
    def _(t):
        in_plane((r + t) % plane).wait_send()

    @pl.loop(1, planes)
    def _(t):
        in_column((z + t) % planes, z).wait_send()


def finish(packed, out_inv, out_sla, out_pos, out_log, out_en, out_mean):
    out_inv[...] = packed[0:256, :]
    out_sla[...] = packed[256:512, :]
    for c in range(3):
        for s in range(2):
            row = 512 + 8 * c + 4 * s
            out_pos[c, :, s * NEL : (s + 1) * NEL] = packed[row : row + 4, :]
    logs, energies = packed[536:544, :], packed[544:552, :]
    for i in range(WD):
        out_log[i] = logs[i, 0]
        out_en[i] = energies[i, 0]
    out_mean[0] = packed[552:560, :][0, 0]


def solution(mesh):
    walkers = mesh.shape["walkers"]
    plane = 16 if walkers == 128 else walkers // 2
    planes = walkers // plane

    def body(
        inverse,
        slater,
        positions,
        displacements,
        move_order,
        accepted,
        counts,
        log_amp,
        centers,
        exponents,
        orbitals,
        jastrow,
    ):
        smem = pl.BlockSpec(memory_space=pltpu.SMEM)
        vmem = pl.BlockSpec(memory_space=pltpu.VMEM)
        hbm = pl.BlockSpec(memory_space=pltpu.HBM)

        def shape(*dims):
            return jax.ShapeDtypeStruct(dims, F32)

        def buf(*dims, kind=F32):
            return pltpu.VMEM(dims, kind)

        dma = pltpu.SemaphoreType.DMA
        packed = pl.pallas_call(
            lambda *refs: kernel(planes, plane, *refs),
            out_shape=shape(560, 128),
            in_specs=[hbm] * 12,
            out_specs=vmem,
            scratch_shapes=[
                pltpu.SMEM((4,), jnp.int32),
                pltpu.SMEM((4,), F32),
                pltpu.SMEM((4,), F32),
                buf(256, 128),
                buf(256, 128),
                buf(3, 4, 256),
                buf(3, 4, 256),
                buf(8, 128, kind=jnp.int32),
                buf(8, 32, kind=jnp.int32),
                buf(3, 1024),
                buf(8, 128),
                buf(2, 32, 1024),
                buf(2, 128, 1024, kind=BF16),
                buf(2, 128, 1024, kind=BF16),
                buf(256, 128, kind=BF16),
                buf(256, 128, kind=BF16),
                buf(256, 128),
                buf(4, 8, 128),
                buf(4, 16, 128),
                buf(6, 256, 128),
                buf(32, 128),
                buf(128, 128),
                buf(128, 128),
                buf(128, 128),
                buf(128, 128),
                buf(2, 136, 128),
                *[buf(144, 128) for _ in range(8)],
                buf(1, 128),
                buf(1, 128),
                buf(plane, 1, 128),
                buf(planes, 1, 128),
                dma((12,)),
                dma((7,)),
                dma((7,)),
                dma((plane,)),
                dma((plane,)),
                dma((planes,)),
                dma((planes,)),
            ],
            compiler_params=pltpu.CompilerParams(
                collective_id=0, has_side_effects=True, vmem_limit_bytes=16 << 20
            ),
            name="generation",
        )(*[pltpu.with_memory_space_constraint(x, pltpu.HBM) for x in (
            counts,
            jastrow,
            log_amp,
            inverse.reshape(256, 128),
            slater.reshape(256, 128),
            positions.transpose(1, 0, 2),
            displacements.transpose(1, 0, 2),
            move_order.reshape(8, 128),
            accepted.reshape(8, 32),
            centers,
            exponents.reshape(8, 128),
            orbitals,
        )])
        outs = pl.pallas_call(
            finish,
            out_shape=(
                shape(256, 128),
                shape(256, 128),
                shape(3, 4, 256),
                shape(4),
                shape(4),
                shape(1),
            ),
            in_specs=[vmem],
            out_specs=(vmem, vmem, vmem, smem, smem, smem),
            compiler_params=pltpu.CompilerParams(vmem_limit_bytes=4 << 20),
            name="finish",
        )(packed)
        return (
            outs[0].reshape(4, 2, 32, 128),
            outs[1].reshape(4, 2, 32, 128),
            outs[2].transpose(1, 0, 2),
            outs[3],
            outs[4],
            outs[5].reshape(()),
        )

    placed = (
        P("walkers", None, "orb", None),
        P("walkers", None, "orb", None),
        P("walkers", None, None),
        P("walkers", None, None),
        P("walkers", None, None),
        P("walkers", None, None),
        P("walkers"),
        P("walkers"),
        P(),
        P(),
        P(None, "orb", None),
        P(),
    )
    return jax.shard_map(
        body,
        mesh=mesh,
        in_specs=placed,
        out_specs=(
            P("walkers", None, "orb", None),
            P("walkers", None, "orb", None),
            P("walkers", None, None),
            P("walkers"),
            P("walkers"),
            P(),
        ),
        check_vma=False,
    )
```

```python
import math

import jax
import jax.numpy as jnp
from jax import lax
from jax.experimental import pallas as pl
from jax.experimental.pallas import tpu as pltpu
from jax.sharding import PartitionSpec as P

NEL = 128
K = 32
WD = 4
F32 = jnp.float32
BF16 = jnp.bfloat16
MESH = pl.DeviceIdType.MESH
LOG2E = math.log2(math.e)


def split(x):
    high = x.astype(BF16)
    return high, (x - high.astype(F32)).astype(BF16)


def product(a, b, dims):
    return lax.dot_general(a, b, (dims, ((), ())), preferred_element_type=F32)


NN = ((1,), (0,))
NT = ((1,), (1,))
TN = ((0,), (0,))


def product3(a, b, dims=NN):
    ah, al = a
    bh, bl = b
    return product(ah, bh, dims) + product(ah, bl, dims) + product(al, bh, dims)


def iota(shape, dim):
    return lax.broadcasted_iota(jnp.int32, shape, dim)


def flag(cond):
    return jnp.full((8, 128), cond.astype(jnp.int32), jnp.int32) == 1


def splat(x):
    return jnp.broadcast_to(x, (8, 128))


def pick(mask, new, old):
    rows = new.shape[0]
    new3, old3 = new.reshape(rows // 8, 8, 128), old.reshape(rows // 8, 8, 128)
    return jnp.where(mask[None], new3, old3).reshape(rows, 128)


def kernel(
    planes,
    plane,
    cnt_hbm,
    jas_hbm,
    amp_hbm,
    inv_hbm,
    sla_hbm,
    pos_hbm,
    dis_hbm,
    mo_hbm,
    acc_hbm,
    cen_hbm,
    ex_hbm,
    orb_hbm,
    out,
    counts,
    jastrow,
    log_amp,
    inv,
    sla,
    pos,
    dis,
    mo,
    acc,
    cen,
    ex,
    orb,
    dhi,
    dlo,
    oh,
    oha,
    ac,
    misc,
    here,
    pts,
    logt,
    snd_a,
    part,
    rcv_a,
    rcv_b,
    solv,
    sla_r,
    sla_l,
    rs_r,
    rs_l,
    inv_r,
    inv_l,
    ri_r,
    ri_l,
    row_a,
    row_b,
    pre,
    tab_a,
    tab_b,
    in_sem,
    send_x,
    recv_x,
    send_a,
    recv_a,
    send_b,
    recv_b,
    up_sem,
):
    me = lax.axis_index("walkers")
    ob = lax.axis_index("orb")
    walkers = planes * plane
    core = ob % 2
    partner = (ob // 2) * 2 + (1 - core)
    across = (1 - ob // 2) * 2 + core
    z, r = me // plane, me % plane

    def at(w, o):
        return {"walkers": w, "orb": o}

    barrier = pltpu.get_barrier_semaphore()

    def greet(w, o):
        pl.semaphore_signal(barrier, inc=1, device_id=at(w, o), device_id_type=MESH)

    greet(me, partner)
    greet(me, across)
    has_right, has_left = me < walkers - 1, me > 0

    @pl.when(has_right)
    def _():
        greet(me + 1, ob)

    @pl.when(has_left)
    def _():
        greet(me - 1, ob)

    for t in range(1, plane):
        greet(z * plane + (r + t) % plane, ob)

    for q in range(1, planes):
        @pl.when(q > z)
        def _(q=q):
            greet(q * plane + r, ob)

    loads = [
        pltpu.make_async_copy(src, dst, in_sem.at[n])
        for n, (src, dst) in enumerate(
            (
                (mo_hbm, mo),
                (acc_hbm, acc),
                (pos_hbm, pos),
                (dis_hbm, dis),
                (cen_hbm, cen),
                (ex_hbm, ex),
                (cnt_hbm, counts),
                (jas_hbm, jastrow),
                (amp_hbm, log_amp),
                (orb_hbm, orb),
                (inv_hbm, inv),
                (sla_hbm, sla),
            )
        )
    ]
    for load in loads:
        load.start()
    @pl.when(me == 0)
    def _():
        rs_l[...] = jnp.zeros_like(rs_l)
        ri_l[...] = jnp.zeros_like(ri_l)

    @pl.when(me == walkers - 1)
    def _():
        rs_r[...] = jnp.zeros_like(rs_r)
        ri_r[...] = jnp.zeros_like(ri_r)

    late = z >= planes // 2
    early = jnp.logical_not(late)
    eager = late & (r >= 2)
    patient = jnp.logical_not(eager)

    def enter():
        neighbours = jnp.where(has_right, 1, 0) + jnp.where(has_left, 1, 0)
        pl.semaphore_wait(barrier, 2 + (plane - 1) + z + neighbours)

        @pl.loop(0, planes)
        def _(q):
            @pl.when(q < z)
            def _():
                pl.semaphore_signal(
                    up_sem.at[z],
                    inc=1,
                    device_id=at(q * plane + r, ob),
                    device_id_type=MESH,
                )

    for load in loads[:6]:
        load.wait()

    for w in range(WD):
        for c in range(3):
            for s in range(2):
                cols = slice(s * NEL, (s + 1) * NEL)
                n = 2 * c + s
                here[w, n : n + 1, :] = pos[c, w : w + 1, cols]
                here[w, n + 8 : n + 9, :] = dis[c, w : w + 1, cols]

    lane = iota((K, 128), 1)
    diag = lane == iota((K, 128), 0)

    @pl.loop(0, 2 * WD)
    def _(b):
        w, s = b // 2, b % 2
        order = mo[pl.ds(b, 1), :].astype(F32)
        taken = acc[pl.ds(b, 1), :].astype(F32)
        ek = jnp.sum(jnp.where(diag, order, 0.0), axis=1, keepdims=True)
        ak = jnp.sum(
            jnp.where(diag[:, :K], taken, 0.0), axis=1, keepdims=True
        )
        one = jnp.where(lane.astype(F32) == ek, 1.0, 0.0)
        took = one * ak
        rows = pl.ds(pl.multiple_of(b * K, K), K)
        oh[rows, :] = one.astype(BF16)
        oha[rows, :] = took.astype(BF16)
        ac[rows, :] = jnp.broadcast_to(ak, (K, 128))
        applied = jnp.sum(took, axis=0, keepdims=True)
        old, new = [], []
        for c in range(3):
            p = here[w, pl.ds(2 * c + s, 1), :]
            d = here[w, pl.ds(2 * c + s + 8, 1), :]
            old.append(jnp.sum(one * p, axis=1, keepdims=True))
            new.append(jnp.sum(one * (p + d), axis=1, keepdims=True))
            misc[w, pl.ds(2 * c + s, 1), :] = p + d * applied
        for c in range(3):
            pts[c, rows, :] = jnp.broadcast_to(old[c], (K, 128))
            pts[c + 3, rows, :] = jnp.broadcast_to(new[c], (K, 128))

    for load in loads[6:9]:
        load.wait()
    sub32 = iota((32, 128), 0)

    l1 = iota((1, 128), 1)
    c = [counts[n] for n in range(WD)]
    limit = [c[0]]
    for n in range(1, WD):
        limit.append(limit[-1] + c[n])
    start = [limit[n] - c[n] for n in range(WD)]
    total = limit[-1]
    def columns(ref, w, si, n):
        on = lane == sub32 + 32 * n
        got = []
        for c in range(3):
            row = ref[w, 2 * c + si : 2 * c + si + 1, :]
            got.append(jnp.sum(jnp.where(on, row, 0.0), axis=1, keepdims=True))
        return got

    def squares(column, ref, w, sj):
        out = jnp.zeros((32, 128), F32)
        for c in range(3):
            d = column[c] - ref[w, 2 * c + sj : 2 * c + sj + 1, :]
            out = out + d * d
        return out

    def whole(x):
        return jnp.sum(jnp.sum(x, axis=0, keepdims=True), axis=1, keepdims=True)

    def energies():
        @pl.loop(0, WD, unroll=True)
        def _(w):
            es = jnp.zeros((32, 128), F32)
            ed = jnp.zeros((32, 128), F32)
            for si in range(2):
                for n in range(4):
                    column = columns(misc, w, si, n)
                    es = es + lax.rsqrt(squares(column, misc, w, si) + 1.0)
                    if si == 0:
                        ed = ed + lax.rsqrt(squares(column, misc, w, 1) + 1.0)
            energy = (whole(es + 2.0 * ed) - 2.0 * NEL) / (2.0 * NEL * (2 * NEL - 1))
            misc[w, 6:7, :] = jnp.broadcast_to(energy, (1, 128))

        weighted = jnp.zeros((1, 128), F32)
        for n in range(WD):
            weighted = weighted + c[n].astype(F32) * misc[n, 6:7, :]
        own = jnp.where(l1 == 0, total.astype(F32), jnp.where(l1 == 1, weighted, 0.0))
        row_a[...] = own

    def jastrow_change():
        @pl.loop(0, WD)
        def _(w):
            def change_of(oc, nc, sj, falloff):
                od = jnp.sqrt(squares(oc, here, w, sj))
                nd = jnp.sqrt(squares(nc, misc, w, sj))
                return (nd - od) / ((1.0 + falloff * nd) * (1.0 + falloff * od))

            js = jnp.zeros((32, 128), F32)
            jd = jnp.zeros((32, 128), F32)
            for si in range(2):
                for n in range(4):
                    oc, nc = columns(here, w, si, n), columns(misc, w, si, n)
                    js = js + change_of(oc, nc, si, jastrow[2])
                    if si == 0:
                        jd = jd + change_of(oc, nc, 1, jastrow[3])
            jt = whole(jastrow[0] * js + (2.0 * jastrow[1]) * jd)
            misc[w, 7:8, :] = jnp.broadcast_to(jt, (1, 128))

    def in_plane(q):
        return pltpu.make_async_remote_copy(
            src_ref=row_a,
            dst_ref=tab_a.at[r],
            send_sem=send_a.at[q],
            recv_sem=recv_a.at[r],
            device_id=at(z * plane + q, ob),
            device_id_type=MESH,
        )

    def from_plane(q):
        return pltpu.make_async_remote_copy(
            src_ref=row_a,
            dst_ref=tab_a.at[q],
            send_sem=send_a.at[q],
            recv_sem=recv_a.at[q],
            device_id=at(z * plane + q, ob),
            device_id_type=MESH,
        )

    def send_plane():
        @pl.loop(1, plane)
        def _(t):
            in_plane((r + t) % plane).start()


    def table(tab, rows, place, own_row):
        before = jnp.zeros((1, 128), F32)
        every = jnp.zeros((1, 128), F32)
        for n in range(rows):
            x = jnp.where(jnp.full((1, 128), place, jnp.int32) == n, own_row, tab[n])
            before = before + jnp.where(jnp.full((1, 128), place, jnp.int32) > n, x, 0.0)
            every = every + x
        return before, every

    def in_column(q, slot):
        return pltpu.make_async_remote_copy(
            src_ref=row_b,
            dst_ref=tab_b.at[slot],
            send_sem=send_b.at[q],
            recv_sem=recv_b.at[slot],
            device_id=at(q * plane + r, ob),
            device_id_type=MESH,
        )

    def send_column():
        @pl.loop(1, plane)
        def _(t):
            from_plane((r + t) % plane).wait_recv()

        pre[...], row_b[...] = table(tab_a, plane, r, row_a[...])

        @pl.loop(0, planes)
        def _(q):
            @pl.when(q < z)
            def _():
                in_column(q, z).start()

    energies()

    @pl.when(eager)
    def _():
        enter()
        send_plane()

    @pl.loop(0, 2 * WD)
    def _(b):
        w, s = b // 2, b % 2
        rows = pl.ds(pl.multiple_of(b * K, K), K)
        old = [pts[c, rows, :] for c in range(3)]
        new = [pts[c + 3, rows, :] for c in range(3)]
        to = pl.ds(pl.multiple_of(w * K, K), K)
        for n in range(8):
            span = slice(n * 128, (n + 1) * 128)
            rate = ex[n : n + 1, :] * (-LOG2E)
            far = jnp.zeros((K, 128), F32)
            near = jnp.zeros((K, 128), F32)
            for c in range(3):
                center = cen[c : c + 1, span]
                a, e = old[c] - center, new[c] - center
                far = far + a * a
                near = near + e * e
            differ = jnp.exp2(rate * near) - jnp.exp2(rate * far)
            high, low = split(differ)
            dhi[s, to, span] = high
            dlo[s, to, span] = low

    @pl.when(patient)
    def _():
        enter()
        send_plane()

    loads[9].wait()
    shift = []
    for s in range(2):
        high, low = split(orb[s])
        high4 = jnp.concatenate([high] * 4, axis=0)
        low4 = jnp.concatenate([low] * 4, axis=0)
        a = dhi[s]
        shift.append(product(a, high4, NT) + product(a, low4, NT) + product(dlo[s], high4, NT))

    seg = iota((K, 128), 1) // K

    def block_rows(parts):
        return jnp.concatenate(
            [jnp.where(seg == n, x, 0.0) for n, x in enumerate(parts)], axis=0
        )

    shift_blocks = []
    for g in range(2):
        shift_blocks.append(
            split(
                block_rows(
                    [
                        shift[b % 2][(2 * g + b // 2) * K : (2 * g + b // 2 + 1) * K]
                        for b in range(4)
                    ]
                )
            )
        )

    loads[10].wait()
    change = []
    for g in range(2):
        rows = slice(g * 128, (g + 1) * 128)
        full = product3(shift_blocks[g], split(inv[rows, :]))
        change.append(jnp.where(ac[rows, :] > 0.5, full, 0.0))
    first = core == 0
    mine_mask = flag(first)
    snd_a[...] = pick(mine_mask, change[1], change[0])
    part[...] = pick(mine_mask, change[0], change[1])

    def remote(src, dst, n, w, o):
        return pltpu.make_async_remote_copy(
            src_ref=src,
            dst_ref=dst,
            send_sem=send_x.at[n],
            recv_sem=recv_x.at[n],
            device_id=at(w, o),
            device_id_type=MESH,
        )

    to_partner = remote(snd_a, rcv_a, 0, me, partner)

    to_partner.start()

    loads[11].wait()
    sla_now = []
    for g in range(2):
        rows = slice(g * 128, (g + 1) * 128)
        high, low = shift_blocks[g]
        taken = oha[rows, :]
        added = product(high, taken, TN) + product(low, taken, TN)
        sla[rows, :] = sla[rows, :] + added

    to_partner.wait_recv()
    part[...] = part[...] + rcv_a[...]
    to_across = remote(part, rcv_b, 1, me, across)
    to_across.start()

    @pl.when(late)
    def _():
        send_column()

    jastrow_change()

    tiles = [misc[n] for n in range(WD)]

    def copy_masks(j):
        return [flag((start[n] <= j) & (j < limit[n])) for n in range(WD)]

    right_masks = [copy_masks(total - 1), copy_masks(total - 2)]
    left_masks = [copy_masks(jnp.int32(0)), copy_masks(jnp.int32(1))]

    def chosen(masks, parts):
        out = jnp.zeros_like(parts[0])
        for m, x in zip(masks, parts):
            out = pick(m, x, out)
        return out

    def pack(dst, masks, parts, n_rows):
        for n in range(2):
            dst[n * n_rows : (n + 1) * n_rows, :] = chosen(masks[n], parts)

    slaters = [sla[n * 64 : (n + 1) * 64, :] for n in range(WD)]
    pack(sla_r, right_masks, slaters, 64)
    pack(sla_l, left_masks, slaters, 64)
    for n in range(2):
        sla_r[128 + 8 * n : 136 + 8 * n, :] = chosen(right_masks[n], tiles)
        sla_l[128 + 8 * n : 136 + 8 * n, :] = chosen(left_masks[n], tiles)

    column_blocks = []
    block_on = (iota((128, 128), 0) // K) == (iota((128, 128), 1) // K)
    for g in range(2):
        rows = slice(g * 128, (g + 1) * 128)
        high, low = split(inv[rows, :])
        which = oh[rows, :]
        got = product(high, which, NT) + product(low, which, NT)
        column_blocks.append(split(jnp.where(block_on, got, 0.0)))

    slater_right = remote(sla_r, rs_l, 3, me + 1, ob)
    slater_left = remote(sla_l, rs_r, 4, me - 1, ob)

    def start_both(to_right, to_left):
        @pl.when(has_right)
        def _():
            to_right.start()

        @pl.when(has_left)
        def _():
            to_left.start()

    to_across.wait_recv()
    start_both(slater_right, slater_left)
    summed = part[...] + rcv_b[...]
    high, low = split(summed)
    which = oh[pl.ds(pl.multiple_of(core * 128, 128), 128), :]
    got = product(high, which, NT) + product(low, which, NT)
    lane8 = iota((8, 128), 1)
    sub8 = iota((8, 128), 0)
    seg8 = lane8 // K
    in_seg = lane8 % K
    tile = []
    for t in range(4):
        x = jnp.where(in_seg == sub8 + 8 * t, 1.0, 0.0)
        for b in range(4):
            x = x + jnp.where(seg8 == b, got[b * K + 8 * t : b * K + 8 * t + 8], 0.0)
        tile.append(x)

    def panel(p, carry):
        m, logs = list(carry[:4]), carry[4]
        base = 8 * p
        cols = [
            [jnp.take_along_axis(m[t], seg8 * K + base + n, axis=1) for t in range(4)]
            for n in range(8)
        ]
        pivots = jnp.ones((8, 128), F32)
        for n in range(8):
            bk = cols[n]
            pivot = bk[0][n : n + 1, :]
            inverse_pivot = 1.0 / pivot
            pivots = jnp.where(sub8 == n, pivot, pivots)
            spot = in_seg == base + n
            row = jnp.where(spot, inverse_pivot, m[0][n : n + 1, :] * inverse_pivot)
            for t in range(4):
                fresh = jnp.where(spot, 0.0, m[t]) - bk[t] * row
                m[t] = jnp.where(sub8 == n, row, fresh) if t == 0 else fresh
            for j in range(n + 1, 8):
                scale = cols[j][0][n : n + 1, :] * inverse_pivot
                for t in range(4):
                    fresh = cols[j][t] - bk[t] * scale
                    cols[j][t] = jnp.where(sub8 == n, scale, fresh) if t == 0 else fresh
        logs = logs + jnp.log(jnp.abs(pivots))
        return m[1], m[2], m[3], m[0], logs

    *tile, logs = lax.fori_loop(0, 4, panel, (*tile, jnp.zeros((8, 128), F32)))
    reverse = jnp.concatenate(tile, axis=0)
    solved = product3(split(block_rows([reverse] * 4)), (high, low))
    logdet = jnp.broadcast_to(jnp.sum(logs, axis=0, keepdims=True), (8, 128))
    solv[core, 0:128, :] = solved
    solv[core, 128:136, :] = logdet
    swap = remote(solv.at[core], solv.at[core], 2, me, partner)
    swap.start()

    @pl.when(early)
    def _():
        send_column()

    swap_in = remote(solv.at[1 - core], solv.at[1 - core], 2, me, partner)
    swap_in.wait_recv()
    for g in range(2):
        rows = slice(g * 128, (g + 1) * 128)
        inv[rows, :] = inv[rows, :] - product3(column_blocks[g], split(solv[g, 0:128, :]))
    for n in range(WD):
        row = solv[n // 2, 128:136, :]
        base = 64 * (n % 2)
        up_down = jnp.where((lane8 == base) | (lane8 == base + K), row, 0.0)
        both = splat(jnp.sum(up_down, axis=1, keepdims=True))
        logt[8 * n : 8 * n + 8, :] = (log_amp[n] + both) + 0.5 * splat(tiles[n][7:8, :])
    inverses = [inv[n * 64 : (n + 1) * 64, :] for n in range(WD)]
    log_tiles = [logt[8 * n : 8 * n + 8, :] for n in range(WD)]
    pack(inv_r, right_masks, inverses, 64)
    pack(inv_l, left_masks, inverses, 64)
    for n in range(2):
        inv_r[128 + 8 * n : 136 + 8 * n, :] = chosen(right_masks[n], log_tiles)
        inv_l[128 + 8 * n : 136 + 8 * n, :] = chosen(left_masks[n], log_tiles)
    inverse_right = remote(inv_r, ri_l, 5, me + 1, ob)
    inverse_left = remote(inv_l, ri_r, 6, me - 1, ob)
    start_both(inverse_right, inverse_left)

    @pl.loop(1, planes)
    def _(t):
        @pl.when(z + t < planes)
        def _():
            pl.semaphore_wait(up_sem.at[z + t], 1)
            in_column(z + t, z).start()

    @pl.loop(1, planes)
    def _(t):
        q = (z + t) % planes
        in_column(q, q).wait_recv()

    every_a, before_a = row_b[...], pre[...]

    before_b, every_b = table(tab_b, planes, z, every_a)
    mean = jnp.sum(jnp.where(l1 == 1, every_b, 0.0), axis=1, keepdims=True)
    out[552:560, :] = splat(mean) / (WD * walkers)
    ahead = jnp.where(l1 == 0, before_a + before_b, 0.0)
    over = splat(jnp.sum(ahead, axis=1, keepdims=True)) - (WD * me).astype(F32)

    @pl.when(has_left)
    def _():
        slater_right.wait_recv()
        inverse_right.wait_recv()

    @pl.when(has_right)
    def _():
        slater_left.wait_recv()
        inverse_left.wait_recv()

    totalf = total.astype(F32)
    for i in range(WD):
        j = i - over
        masks = [j == -1.0, j == -2.0]
        masks += [
            (j >= start[n].astype(F32)) & (j < limit[n].astype(F32)) for n in range(WD)
        ]
        masks += [j == totalf, j == totalf + 1.0]

        def halo(ref_l, ref_r, n_rows, base):
            return [ref_l[base + n * n_rows : base + (n + 1) * n_rows, :] for n in range(2)], [
                ref_r[base + n * n_rows : base + (n + 1) * n_rows, :] for n in range(2)
            ]

        def select(own_parts, ref_l, ref_r, n_rows, base):
            a, e = halo(ref_l, ref_r, n_rows, base)
            return chosen(masks, a + own_parts + e)

        out[i * 64 : (i + 1) * 64, :] = select(
            [inv[n * 64 : (n + 1) * 64, :] for n in range(WD)], ri_l, ri_r, 64, 0
        )
        out[256 + i * 64 : 256 + (i + 1) * 64, :] = select(
            [sla[n * 64 : (n + 1) * 64, :] for n in range(WD)], rs_l, rs_r, 64, 0
        )
        small = select([misc[n] for n in range(WD)], rs_l, rs_r, 8, 128)
        logs_here = select(
            [logt[8 * n : 8 * n + 8, :] for n in range(WD)], ri_l, ri_r, 8, 128
        )
        for n in range(6):
            row = 512 + 4 * n + i
            out[row : row + 1, :] = small[n : n + 1, :]
        out[536 + i : 537 + i, :] = logs_here[0:1, :]
        out[544 + i : 545 + i, :] = small[6:7, :]

    for copy in (
        to_partner,
        to_across,
        swap,
    ):
        copy.wait_send()

    @pl.when(has_right)
    def _():
        slater_right.wait_send()
        inverse_right.wait_send()

    @pl.when(has_left)
    def _():
        slater_left.wait_send()
        inverse_left.wait_send()

    @pl.loop(1, plane)
    def _(t):
        in_plane((r + t) % plane).wait_send()

    @pl.loop(1, planes)
    def _(t):
        in_column((z + t) % planes, z).wait_send()


def finish(packed, out_inv, out_sla, out_pos, out_log, out_en, out_mean):
    out_inv[...] = packed[0:256, :]
    out_sla[...] = packed[256:512, :]
    for c in range(3):
        for s in range(2):
            row = 512 + 8 * c + 4 * s
            out_pos[c, :, s * NEL : (s + 1) * NEL] = packed[row : row + 4, :]
    logs, energies = packed[536:544, :], packed[544:552, :]
    for i in range(WD):
        out_log[i] = logs[i, 0]
        out_en[i] = energies[i, 0]
    out_mean[0] = packed[552:560, :][0, 0]


def solution(mesh):
    walkers = mesh.shape["walkers"]
    plane = 16 if walkers == 128 else walkers // 2
    planes = walkers // plane

    def body(
        inverse,
        slater,
        positions,
        displacements,
        move_order,
        accepted,
        counts,
        log_amp,
        centers,
        exponents,
        orbitals,
        jastrow,
    ):
        smem = pl.BlockSpec(memory_space=pltpu.SMEM)
        vmem = pl.BlockSpec(memory_space=pltpu.VMEM)
        hbm = pl.BlockSpec(memory_space=pltpu.HBM)

        def shape(*dims):
            return jax.ShapeDtypeStruct(dims, F32)

        def buf(*dims, kind=F32):
            return pltpu.VMEM(dims, kind)

        dma = pltpu.SemaphoreType.DMA
        packed = pl.pallas_call(
            lambda *refs: kernel(planes, plane, *refs),
            out_shape=shape(560, 128),
            in_specs=[hbm] * 12,
            out_specs=vmem,
            scratch_shapes=[
                pltpu.SMEM((4,), jnp.int32),
                pltpu.SMEM((4,), F32),
                pltpu.SMEM((4,), F32),
                buf(256, 128),
                buf(256, 128),
                buf(3, 4, 256),
                buf(3, 4, 256),
                buf(8, 128, kind=jnp.int32),
                buf(8, 32, kind=jnp.int32),
                buf(3, 1024),
                buf(8, 128),
                buf(2, 32, 1024),
                buf(2, 128, 1024, kind=BF16),
                buf(2, 128, 1024, kind=BF16),
                buf(256, 128, kind=BF16),
                buf(256, 128, kind=BF16),
                buf(256, 128),
                buf(4, 8, 128),
                buf(4, 16, 128),
                buf(6, 256, 128),
                buf(32, 128),
                buf(128, 128),
                buf(128, 128),
                buf(128, 128),
                buf(128, 128),
                buf(2, 136, 128),
                *[buf(144, 128) for _ in range(8)],
                buf(1, 128),
                buf(1, 128),
                buf(1, 128),
                buf(plane, 1, 128),
                buf(planes, 1, 128),
                dma((12,)),
                dma((7,)),
                dma((7,)),
                dma((plane,)),
                dma((plane,)),
                dma((planes,)),
                dma((planes,)),
                pltpu.SemaphoreType.REGULAR((planes,)),
            ],
            compiler_params=pltpu.CompilerParams(
                collective_id=0, has_side_effects=True, vmem_limit_bytes=16 << 20
            ),
            name="generation",
        )(*[pltpu.with_memory_space_constraint(x, pltpu.HBM) for x in (
            counts,
            jastrow,
            log_amp,
            inverse.reshape(256, 128),
            slater.reshape(256, 128),
            positions.transpose(1, 0, 2),
            displacements.transpose(1, 0, 2),
            move_order.reshape(8, 128),
            accepted.reshape(8, 32),
            centers,
            exponents.reshape(8, 128),
            orbitals,
        )])
        outs = pl.pallas_call(
            finish,
            out_shape=(
                shape(256, 128),
                shape(256, 128),
                shape(3, 4, 256),
                shape(4),
                shape(4),
                shape(1),
            ),
            in_specs=[vmem],
            out_specs=(vmem, vmem, vmem, smem, smem, smem),
            compiler_params=pltpu.CompilerParams(vmem_limit_bytes=4 << 20),
            name="finish",
        )(packed)
        return (
            outs[0].reshape(4, 2, 32, 128),
            outs[1].reshape(4, 2, 32, 128),
            outs[2].transpose(1, 0, 2),
            outs[3],
            outs[4],
            outs[5].reshape(()),
        )

    placed = (
        P("walkers", None, "orb", None),
        P("walkers", None, "orb", None),
        P("walkers", None, None),
        P("walkers", None, None),
        P("walkers", None, None),
        P("walkers", None, None),
        P("walkers"),
        P("walkers"),
        P(),
        P(),
        P(None, "orb", None),
        P(),
    )
    return jax.shard_map(
        body,
        mesh=mesh,
        in_specs=placed,
        out_specs=(
            P("walkers", None, "orb", None),
            P("walkers", None, "orb", None),
            P("walkers", None, None),
            P("walkers"),
            P("walkers"),
            P(),
        ),
        check_vma=False,
    )
```

```python
import math

import jax
import jax.numpy as jnp
from jax import lax
from jax.experimental import pallas as pl
from jax.experimental.pallas import tpu as pltpu
from jax.sharding import PartitionSpec as P

NEL = 128
K = 32
WD = 4
F32 = jnp.float32
BF16 = jnp.bfloat16
MESH = pl.DeviceIdType.MESH
LOG2E = math.log2(math.e)


def split(x):
    high = x.astype(BF16)
    return high, (x - high.astype(F32)).astype(BF16)


def product(a, b, dims):
    return lax.dot_general(a, b, (dims, ((), ())), preferred_element_type=F32)


NN = ((1,), (0,))
NT = ((1,), (1,))
TN = ((0,), (0,))


def product3(a, b, dims=NN):
    ah, al = a
    bh, bl = b
    return product(ah, bh, dims) + product(ah, bl, dims) + product(al, bh, dims)


def iota(shape, dim):
    return lax.broadcasted_iota(jnp.int32, shape, dim)


def flag(cond):
    return jnp.full((8, 128), cond.astype(jnp.int32), jnp.int32) == 1


def splat(x):
    return jnp.broadcast_to(x, (8, 128))


def pick(mask, new, old):
    rows = new.shape[0]
    new3, old3 = new.reshape(rows // 8, 8, 128), old.reshape(rows // 8, 8, 128)
    return jnp.where(mask[None], new3, old3).reshape(rows, 128)


def kernel(
    planes,
    plane,
    cnt_hbm,
    jas_hbm,
    amp_hbm,
    inv_hbm,
    sla_hbm,
    pos_hbm,
    dis_hbm,
    mo_hbm,
    acc_hbm,
    cen_hbm,
    ex_hbm,
    orb_hbm,
    out,
    counts,
    jastrow,
    log_amp,
    inv,
    sla,
    pos,
    dis,
    mo,
    acc,
    cen,
    ex,
    orb,
    dhi,
    dlo,
    oh,
    oha,
    ac,
    misc,
    here,
    pts,
    logt,
    snd_a,
    part,
    rcv_a,
    rcv_b,
    solv,
    sla_r,
    sla_l,
    rs_r,
    rs_l,
    inv_r,
    inv_l,
    ri_r,
    ri_l,
    row_a,
    row_b,
    pre,
    tab_a,
    tab_b,
    in_sem,
    send_x,
    recv_x,
    send_a,
    recv_a,
    send_b,
    recv_b,
    up_sem,
):
    me = lax.axis_index("walkers")
    ob = lax.axis_index("orb")
    walkers = planes * plane
    core = ob % 2
    partner = (ob // 2) * 2 + (1 - core)
    across = (1 - ob // 2) * 2 + core
    z, r = me // plane, me % plane

    def at(w, o):
        return {"walkers": w, "orb": o}

    loads = [
        pltpu.make_async_copy(src, dst, in_sem.at[n])
        for n, (src, dst) in enumerate(
            (
                (mo_hbm, mo),
                (acc_hbm, acc),
                (pos_hbm, pos),
                (dis_hbm, dis),
                (cen_hbm, cen),
                (ex_hbm, ex),
                (cnt_hbm, counts),
                (jas_hbm, jastrow),
                (amp_hbm, log_amp),
                (orb_hbm, orb),
                (inv_hbm, inv),
                (sla_hbm, sla),
            )
        )
    ]
    for load in loads:
        load.start()
    barrier = pltpu.get_barrier_semaphore()

    def greet(w, o):
        pl.semaphore_signal(barrier, inc=1, device_id=at(w, o), device_id_type=MESH)

    greet(me, partner)
    greet(me, across)
    has_right, has_left = me < walkers - 1, me > 0

    @pl.when(has_right)
    def _():
        greet(me + 1, ob)

    @pl.when(has_left)
    def _():
        greet(me - 1, ob)

    for t in range(1, plane):
        greet(z * plane + (r + t) % plane, ob)

    for q in range(1, planes):
        @pl.when(q > z)
        def _(q=q):
            greet(q * plane + r, ob)

    @pl.when(me == 0)
    def _():
        rs_l[...] = jnp.zeros_like(rs_l)
        ri_l[...] = jnp.zeros_like(ri_l)

    @pl.when(me == walkers - 1)
    def _():
        rs_r[...] = jnp.zeros_like(rs_r)
        ri_r[...] = jnp.zeros_like(ri_r)

    late = z >= planes // 2
    early = jnp.logical_not(late)
    eager = late & (r >= 2)
    patient = jnp.logical_not(eager)

    def enter():
        neighbours = jnp.where(has_right, 1, 0) + jnp.where(has_left, 1, 0)
        pl.semaphore_wait(barrier, 2 + (plane - 1) + z + neighbours)

        @pl.loop(0, planes)
        def _(q):
            @pl.when(q < z)
            def _():
                pl.semaphore_signal(
                    up_sem.at[z],
                    inc=1,
                    device_id=at(q * plane + r, ob),
                    device_id_type=MESH,
                )

    for load in loads[:6]:
        load.wait()

    for w in range(WD):
        for c in range(3):
            for s in range(2):
                cols = slice(s * NEL, (s + 1) * NEL)
                n = 2 * c + s
                here[w, n : n + 1, :] = pos[c, w : w + 1, cols]
                here[w, n + 8 : n + 9, :] = dis[c, w : w + 1, cols]

    lane = iota((K, 128), 1)
    diag = lane == iota((K, 128), 0)

    @pl.loop(0, 2 * WD, unroll=4)
    def _(b):
        w, s = b // 2, b % 2
        order = mo[pl.ds(b, 1), :].astype(F32)
        taken = acc[pl.ds(b, 1), :].astype(F32)
        ek = jnp.sum(jnp.where(diag, order, 0.0), axis=1, keepdims=True)
        ak = jnp.sum(
            jnp.where(diag[:, :K], taken, 0.0), axis=1, keepdims=True
        )
        one = jnp.where(lane.astype(F32) == ek, 1.0, 0.0)
        took = one * ak
        rows = pl.ds(pl.multiple_of(b * K, K), K)
        oh[rows, :] = one.astype(BF16)
        oha[rows, :] = took.astype(BF16)
        ac[rows, :] = jnp.broadcast_to(ak, (K, 128))
        applied = jnp.sum(took, axis=0, keepdims=True)
        old, new = [], []
        for c in range(3):
            p = here[w, pl.ds(2 * c + s, 1), :]
            d = here[w, pl.ds(2 * c + s + 8, 1), :]
            old.append(jnp.sum(one * p, axis=1, keepdims=True))
            new.append(jnp.sum(one * (p + d), axis=1, keepdims=True))
            misc[w, pl.ds(2 * c + s, 1), :] = p + d * applied
        for c in range(3):
            pts[c, rows, :] = jnp.broadcast_to(old[c], (K, 128))
            pts[c + 3, rows, :] = jnp.broadcast_to(new[c], (K, 128))

    for load in loads[6:9]:
        load.wait()
    sub32 = iota((32, 128), 0)

    l1 = iota((1, 128), 1)
    c = [counts[n] for n in range(WD)]
    limit = [c[0]]
    for n in range(1, WD):
        limit.append(limit[-1] + c[n])
    start = [limit[n] - c[n] for n in range(WD)]
    total = limit[-1]
    def columns(ref, w, si, n):
        on = lane == sub32 + 32 * n
        got = []
        for c in range(3):
            row = ref[w, 2 * c + si : 2 * c + si + 1, :]
            got.append(jnp.sum(jnp.where(on, row, 0.0), axis=1, keepdims=True))
        return got

    def squares(column, ref, w, sj):
        out = jnp.zeros((32, 128), F32)
        for c in range(3):
            d = column[c] - ref[w, 2 * c + sj : 2 * c + sj + 1, :]
            out = out + d * d
        return out

    def whole(x):
        return jnp.sum(jnp.sum(x, axis=0, keepdims=True), axis=1, keepdims=True)

    def energies():
        @pl.loop(0, WD, unroll=True)
        def _(w):
            es = jnp.zeros((32, 128), F32)
            ed = jnp.zeros((32, 128), F32)
            for si in range(2):
                for n in range(4):
                    column = columns(misc, w, si, n)
                    es = es + lax.rsqrt(squares(column, misc, w, si) + 1.0)
                    if si == 0:
                        ed = ed + lax.rsqrt(squares(column, misc, w, 1) + 1.0)
            energy = (whole(es + 2.0 * ed) - 2.0 * NEL) / (2.0 * NEL * (2 * NEL - 1))
            misc[w, 6:7, :] = jnp.broadcast_to(energy, (1, 128))

        weighted = jnp.zeros((1, 128), F32)
        for n in range(WD):
            weighted = weighted + c[n].astype(F32) * misc[n, 6:7, :]
        own = jnp.where(l1 == 0, total.astype(F32), jnp.where(l1 == 1, weighted, 0.0))
        row_a[...] = own

    def jastrow_change():
        @pl.loop(0, WD)
        def _(w):
            def change_of(oc, nc, sj, falloff):
                od = jnp.sqrt(squares(oc, here, w, sj))
                nd = jnp.sqrt(squares(nc, misc, w, sj))
                return (nd - od) / ((1.0 + falloff * nd) * (1.0 + falloff * od))

            js = jnp.zeros((32, 128), F32)
            jd = jnp.zeros((32, 128), F32)
            for si in range(2):
                for n in range(4):
                    oc, nc = columns(here, w, si, n), columns(misc, w, si, n)
                    js = js + change_of(oc, nc, si, jastrow[2])
                    if si == 0:
                        jd = jd + change_of(oc, nc, 1, jastrow[3])
            jt = whole(jastrow[0] * js + (2.0 * jastrow[1]) * jd)
            misc[w, 7:8, :] = jnp.broadcast_to(jt, (1, 128))

    def in_plane(q):
        return pltpu.make_async_remote_copy(
            src_ref=row_a,
            dst_ref=tab_a.at[r],
            send_sem=send_a.at[q],
            recv_sem=recv_a.at[r],
            device_id=at(z * plane + q, ob),
            device_id_type=MESH,
        )

    def from_plane(q):
        return pltpu.make_async_remote_copy(
            src_ref=row_a,
            dst_ref=tab_a.at[q],
            send_sem=send_a.at[q],
            recv_sem=recv_a.at[q],
            device_id=at(z * plane + q, ob),
            device_id_type=MESH,
        )

    def send_plane():
        @pl.loop(1, plane)
        def _(t):
            in_plane((r + t) % plane).start()


    def table(tab, rows, place, own_row):
        before = jnp.zeros((1, 128), F32)
        every = jnp.zeros((1, 128), F32)
        for n in range(rows):
            x = jnp.where(jnp.full((1, 128), place, jnp.int32) == n, own_row, tab[n])
            before = before + jnp.where(jnp.full((1, 128), place, jnp.int32) > n, x, 0.0)
            every = every + x
        return before, every

    def in_column(q, slot):
        return pltpu.make_async_remote_copy(
            src_ref=row_b,
            dst_ref=tab_b.at[slot],
            send_sem=send_b.at[q],
            recv_sem=recv_b.at[slot],
            device_id=at(q * plane + r, ob),
            device_id_type=MESH,
        )

    def send_column():
        @pl.loop(1, plane)
        def _(t):
            from_plane((r + t) % plane).wait_recv()

        pre[...], row_b[...] = table(tab_a, plane, r, row_a[...])

        @pl.loop(0, planes)
        def _(q):
            @pl.when(q < z)
            def _():
                in_column(q, z).start()

    energies()

    @pl.when(eager)
    def _():
        enter()
        send_plane()

    loads[9].wait()
    shift = [jnp.zeros((128, 128), F32)] * 2
    for m in range(4):
        for b in range(2 * WD):
            w, s = b // 2, b % 2
            rows, to = slice(b * K, (b + 1) * K), slice(w * K, (w + 1) * K)
            for n in (2 * m, 2 * m + 1):
                span = slice(n * 128, (n + 1) * 128)
                rate = ex[n : n + 1, :] * (-LOG2E)
                far = jnp.zeros((K, 128), F32)
                near = jnp.zeros((K, 128), F32)
                for c3 in range(3):
                    center = cen[c3 : c3 + 1, span]
                    a, e = pts[c3, rows, :] - center, pts[c3 + 3, rows, :] - center
                    far = far + a * a
                    near = near + e * e
                high, low = split(jnp.exp2(rate * near) - jnp.exp2(rate * far))
                dhi[s, to, span] = high
                dlo[s, to, span] = low
        span = slice(m * 256, (m + 1) * 256)
        for s in range(2):
            high, low = split(orb[s, :, span])
            high4 = jnp.concatenate([high] * 4, axis=0)
            low4 = jnp.concatenate([low] * 4, axis=0)
            a = dhi[s, :, span]
            part_sum = product(a, high4, NT) + product(a, low4, NT)
            shift[s] = shift[s] + (part_sum + product(dlo[s, :, span], high4, NT))

    @pl.when(patient)
    def _():
        enter()
        send_plane()

    seg = iota((K, 128), 1) // K

    def block_rows(parts):
        return jnp.concatenate(
            [jnp.where(seg == n, x, 0.0) for n, x in enumerate(parts)], axis=0
        )

    shift_blocks = []
    for g in range(2):
        shift_blocks.append(
            split(
                block_rows(
                    [
                        shift[b % 2][(2 * g + b // 2) * K : (2 * g + b // 2 + 1) * K]
                        for b in range(4)
                    ]
                )
            )
        )

    loads[10].wait()
    change = []
    for g in range(2):
        rows = slice(g * 128, (g + 1) * 128)
        full = product3(shift_blocks[g], split(inv[rows, :]))
        change.append(jnp.where(ac[rows, :] > 0.5, full, 0.0))
    first = core == 0
    mine_mask = flag(first)
    snd_a[...] = pick(mine_mask, change[1], change[0])
    part[...] = pick(mine_mask, change[0], change[1])

    def remote(src, dst, n, w, o):
        return pltpu.make_async_remote_copy(
            src_ref=src,
            dst_ref=dst,
            send_sem=send_x.at[n],
            recv_sem=recv_x.at[n],
            device_id=at(w, o),
            device_id_type=MESH,
        )

    to_partner = remote(snd_a, rcv_a, 0, me, partner)

    to_partner.start()

    loads[11].wait()
    sla_now = []
    for g in range(2):
        rows = slice(g * 128, (g + 1) * 128)
        high, low = shift_blocks[g]
        taken = oha[rows, :]
        added = product(high, taken, TN) + product(low, taken, TN)
        sla[rows, :] = sla[rows, :] + added

    to_partner.wait_recv()
    part[...] = part[...] + rcv_a[...]
    to_across = remote(part, rcv_b, 1, me, across)
    to_across.start()

    @pl.when(late)
    def _():
        send_column()

    jastrow_change()

    tiles = [misc[n] for n in range(WD)]

    def copy_masks(j):
        return [flag((start[n] <= j) & (j < limit[n])) for n in range(WD)]

    right_masks = [copy_masks(total - 1), copy_masks(total - 2)]
    left_masks = [copy_masks(jnp.int32(0)), copy_masks(jnp.int32(1))]

    def chosen(masks, parts):
        out = jnp.zeros_like(parts[0])
        for m, x in zip(masks, parts):
            out = pick(m, x, out)
        return out

    def pack(dst, masks, parts, n_rows):
        for n in range(2):
            dst[n * n_rows : (n + 1) * n_rows, :] = chosen(masks[n], parts)

    slaters = [sla[n * 64 : (n + 1) * 64, :] for n in range(WD)]
    pack(sla_r, right_masks, slaters, 64)
    pack(sla_l, left_masks, slaters, 64)
    for n in range(2):
        sla_r[128 + 8 * n : 136 + 8 * n, :] = chosen(right_masks[n], tiles)
        sla_l[128 + 8 * n : 136 + 8 * n, :] = chosen(left_masks[n], tiles)

    column_blocks = []
    block_on = (iota((128, 128), 0) // K) == (iota((128, 128), 1) // K)
    for g in range(2):
        rows = slice(g * 128, (g + 1) * 128)
        high, low = split(inv[rows, :])
        which = oh[rows, :]
        got = product(high, which, NT) + product(low, which, NT)
        column_blocks.append(split(jnp.where(block_on, got, 0.0)))

    slater_right = remote(sla_r, rs_l, 3, me + 1, ob)
    slater_left = remote(sla_l, rs_r, 4, me - 1, ob)

    def start_both(to_right, to_left):
        @pl.when(has_right)
        def _():
            to_right.start()

        @pl.when(has_left)
        def _():
            to_left.start()

    to_across.wait_recv()
    start_both(slater_right, slater_left)
    summed = part[...] + rcv_b[...]
    high, low = split(summed)
    which = oh[pl.ds(pl.multiple_of(core * 128, 128), 128), :]
    got = product(high, which, NT) + product(low, which, NT)
    lane8 = iota((8, 128), 1)
    sub8 = iota((8, 128), 0)
    seg8 = lane8 // K
    in_seg = lane8 % K
    tile = []
    for t in range(4):
        x = jnp.where(in_seg == sub8 + 8 * t, 1.0, 0.0)
        for b in range(4):
            x = x + jnp.where(seg8 == b, got[b * K + 8 * t : b * K + 8 * t + 8], 0.0)
        tile.append(x)

    def panel(p, carry):
        m, logs = list(carry[:4]), carry[4]
        base = 8 * p
        cols = [
            [jnp.take_along_axis(m[t], seg8 * K + base + n, axis=1) for t in range(4)]
            for n in range(8)
        ]
        pivots = jnp.ones((8, 128), F32)
        for n in range(8):
            bk = cols[n]
            pivot = bk[0][n : n + 1, :]
            inverse_pivot = 1.0 / pivot
            pivots = jnp.where(sub8 == n, pivot, pivots)
            spot = in_seg == base + n
            row = jnp.where(spot, inverse_pivot, m[0][n : n + 1, :] * inverse_pivot)
            for t in range(4):
                fresh = jnp.where(spot, 0.0, m[t]) - bk[t] * row
                m[t] = jnp.where(sub8 == n, row, fresh) if t == 0 else fresh
            for j in range(n + 1, 8):
                scale = cols[j][0][n : n + 1, :] * inverse_pivot
                for t in range(4):
                    fresh = cols[j][t] - bk[t] * scale
                    cols[j][t] = jnp.where(sub8 == n, scale, fresh) if t == 0 else fresh
        logs = logs + jnp.log(jnp.abs(pivots))
        return m[1], m[2], m[3], m[0], logs

    *tile, logs = lax.fori_loop(0, 4, panel, (*tile, jnp.zeros((8, 128), F32)))
    reverse = jnp.concatenate(tile, axis=0)
    solved = product3(split(block_rows([reverse] * 4)), (high, low))
    logdet = jnp.broadcast_to(jnp.sum(logs, axis=0, keepdims=True), (8, 128))
    solv[core, 0:128, :] = solved
    solv[core, 128:136, :] = logdet
    swap = remote(solv.at[core], solv.at[core], 2, me, partner)
    swap.start()

    @pl.when(early)
    def _():
        send_column()

    swap_in = remote(solv.at[1 - core], solv.at[1 - core], 2, me, partner)
    swap_in.wait_recv()
    for g in range(2):
        rows = slice(g * 128, (g + 1) * 128)
        inv[rows, :] = inv[rows, :] - product3(column_blocks[g], split(solv[g, 0:128, :]))
    for n in range(WD):
        row = solv[n // 2, 128:136, :]
        base = 64 * (n % 2)
        up_down = jnp.where((lane8 == base) | (lane8 == base + K), row, 0.0)
        both = splat(jnp.sum(up_down, axis=1, keepdims=True))
        logt[8 * n : 8 * n + 8, :] = (log_amp[n] + both) + 0.5 * splat(tiles[n][7:8, :])
    inverses = [inv[n * 64 : (n + 1) * 64, :] for n in range(WD)]
    log_tiles = [logt[8 * n : 8 * n + 8, :] for n in range(WD)]
    pack(inv_r, right_masks, inverses, 64)
    pack(inv_l, left_masks, inverses, 64)
    for n in range(2):
        inv_r[128 + 8 * n : 136 + 8 * n, :] = chosen(right_masks[n], log_tiles)
        inv_l[128 + 8 * n : 136 + 8 * n, :] = chosen(left_masks[n], log_tiles)
    inverse_right = remote(inv_r, ri_l, 5, me + 1, ob)
    inverse_left = remote(inv_l, ri_r, 6, me - 1, ob)
    start_both(inverse_right, inverse_left)

    @pl.loop(1, planes)
    def _(t):
        @pl.when(z + t < planes)
        def _():
            pl.semaphore_wait(up_sem.at[z + t], 1)
            in_column(z + t, z).start()

    for copy in (
        to_partner,
        to_across,
        swap,
    ):
        copy.wait_send()

    @pl.loop(1, plane)
    def _(t):
        in_plane((r + t) % plane).wait_send()

    @pl.loop(1, planes)
    def _(t):
        q = (z + t) % planes
        in_column(q, q).wait_recv()

    @pl.loop(1, planes)
    def _(t):
        in_column((z + t) % planes, z).wait_send()

    every_a, before_a = row_b[...], pre[...]

    before_b, every_b = table(tab_b, planes, z, every_a)
    mean = jnp.sum(jnp.where(l1 == 1, every_b, 0.0), axis=1, keepdims=True)
    out[552:560, :] = splat(mean) / (WD * walkers)
    ahead = jnp.where(l1 == 0, before_a + before_b, 0.0)
    over = splat(jnp.sum(ahead, axis=1, keepdims=True)) - (WD * me).astype(F32)

    @pl.when(has_left)
    def _():
        slater_right.wait_recv()
        inverse_right.wait_recv()

    @pl.when(has_right)
    def _():
        slater_left.wait_recv()
        inverse_left.wait_recv()

    totalf = total.astype(F32)
    for i in range(WD):
        j = i - over
        masks = [j == -1.0, j == -2.0]
        masks += [
            (j >= start[n].astype(F32)) & (j < limit[n].astype(F32)) for n in range(WD)
        ]
        masks += [j == totalf, j == totalf + 1.0]

        def halo(ref_l, ref_r, n_rows, base):
            return [ref_l[base + n * n_rows : base + (n + 1) * n_rows, :] for n in range(2)], [
                ref_r[base + n * n_rows : base + (n + 1) * n_rows, :] for n in range(2)
            ]

        def select(own_parts, ref_l, ref_r, n_rows, base):
            a, e = halo(ref_l, ref_r, n_rows, base)
            return chosen(masks, a + own_parts + e)

        out[i * 64 : (i + 1) * 64, :] = select(
            [inv[n * 64 : (n + 1) * 64, :] for n in range(WD)], ri_l, ri_r, 64, 0
        )
        out[256 + i * 64 : 256 + (i + 1) * 64, :] = select(
            [sla[n * 64 : (n + 1) * 64, :] for n in range(WD)], rs_l, rs_r, 64, 0
        )
        small = select([misc[n] for n in range(WD)], rs_l, rs_r, 8, 128)
        logs_here = select(
            [logt[8 * n : 8 * n + 8, :] for n in range(WD)], ri_l, ri_r, 8, 128
        )
        for n in range(6):
            row = 512 + 4 * n + i
            out[row : row + 1, :] = small[n : n + 1, :]
        out[536 + i : 537 + i, :] = logs_here[0:1, :]
        out[544 + i : 545 + i, :] = small[6:7, :]

    @pl.when(has_right)
    def _():
        slater_right.wait_send()
        inverse_right.wait_send()

    @pl.when(has_left)
    def _():
        slater_left.wait_send()
        inverse_left.wait_send()


def finish(packed, out_inv, out_sla, out_pos, out_log, out_en, out_mean):
    out_inv[...] = packed[0:256, :]
    out_sla[...] = packed[256:512, :]
    for c in range(3):
        for s in range(2):
            row = 512 + 8 * c + 4 * s
            out_pos[c, :, s * NEL : (s + 1) * NEL] = packed[row : row + 4, :]
    logs, energies = packed[536:544, :], packed[544:552, :]
    for i in range(WD):
        out_log[i] = logs[i, 0]
        out_en[i] = energies[i, 0]
    out_mean[0] = packed[552:560, :][0, 0]


def solution(mesh):
    walkers = mesh.shape["walkers"]
    plane = 16 if walkers == 128 else walkers // 2
    planes = walkers // plane

    def body(
        inverse,
        slater,
        positions,
        displacements,
        move_order,
        accepted,
        counts,
        log_amp,
        centers,
        exponents,
        orbitals,
        jastrow,
    ):
        smem = pl.BlockSpec(memory_space=pltpu.SMEM)
        vmem = pl.BlockSpec(memory_space=pltpu.VMEM)
        hbm = pl.BlockSpec(memory_space=pltpu.HBM)

        def shape(*dims):
            return jax.ShapeDtypeStruct(dims, F32)

        def buf(*dims, kind=F32):
            return pltpu.VMEM(dims, kind)

        dma = pltpu.SemaphoreType.DMA
        packed = pl.pallas_call(
            lambda *refs: kernel(planes, plane, *refs),
            out_shape=shape(560, 128),
            in_specs=[hbm] * 12,
            out_specs=vmem,
            scratch_shapes=[
                pltpu.SMEM((4,), jnp.int32),
                pltpu.SMEM((4,), F32),
                pltpu.SMEM((4,), F32),
                buf(256, 128),
                buf(256, 128),
                buf(3, 4, 256),
                buf(3, 4, 256),
                buf(8, 128, kind=jnp.int32),
                buf(8, 32, kind=jnp.int32),
                buf(3, 1024),
                buf(8, 128),
                buf(2, 32, 1024),
                buf(2, 128, 1024, kind=BF16),
                buf(2, 128, 1024, kind=BF16),
                buf(256, 128, kind=BF16),
                buf(256, 128, kind=BF16),
                buf(256, 128),
                buf(4, 8, 128),
                buf(4, 16, 128),
                buf(6, 256, 128),
                buf(32, 128),
                buf(128, 128),
                buf(128, 128),
                buf(128, 128),
                buf(128, 128),
                buf(2, 136, 128),
                *[buf(144, 128) for _ in range(8)],
                buf(1, 128),
                buf(1, 128),
                buf(1, 128),
                buf(plane, 1, 128),
                buf(planes, 1, 128),
                dma((12,)),
                dma((7,)),
                dma((7,)),
                dma((plane,)),
                dma((plane,)),
                dma((planes,)),
                dma((planes,)),
                pltpu.SemaphoreType.REGULAR((planes,)),
            ],
            compiler_params=pltpu.CompilerParams(
                collective_id=0, has_side_effects=True, vmem_limit_bytes=16 << 20
            ),
            name="generation",
        )(*[pltpu.with_memory_space_constraint(x, pltpu.HBM) for x in (
            counts,
            jastrow,
            log_amp,
            inverse.reshape(256, 128),
            slater.reshape(256, 128),
            positions.transpose(1, 0, 2),
            displacements.transpose(1, 0, 2),
            move_order.reshape(8, 128),
            accepted.reshape(8, 32),
            centers,
            exponents.reshape(8, 128),
            orbitals,
        )])
        outs = pl.pallas_call(
            finish,
            out_shape=(
                shape(256, 128),
                shape(256, 128),
                shape(3, 4, 256),
                shape(4),
                shape(4),
                shape(1),
            ),
            in_specs=[vmem],
            out_specs=(vmem, vmem, vmem, smem, smem, smem),
            compiler_params=pltpu.CompilerParams(vmem_limit_bytes=4 << 20),
            name="finish",
        )(packed)
        return (
            outs[0].reshape(4, 2, 32, 128),
            outs[1].reshape(4, 2, 32, 128),
            outs[2].transpose(1, 0, 2),
            outs[3],
            outs[4],
            outs[5].reshape(()),
        )

    placed = (
        P("walkers", None, "orb", None),
        P("walkers", None, "orb", None),
        P("walkers", None, None),
        P("walkers", None, None),
        P("walkers", None, None),
        P("walkers", None, None),
        P("walkers"),
        P("walkers"),
        P(),
        P(),
        P(None, "orb", None),
        P(),
    )
    return jax.shard_map(
        body,
        mesh=mesh,
        in_specs=placed,
        out_specs=(
            P("walkers", None, "orb", None),
            P("walkers", None, "orb", None),
            P("walkers", None, None),
            P("walkers"),
            P("walkers"),
            P(),
        ),
        check_vma=False,
    )
```

```python
import math

import jax
import jax.numpy as jnp
from jax import lax
from jax.experimental import pallas as pl
from jax.experimental.pallas import tpu as pltpu
from jax.sharding import PartitionSpec as P

NEL = 128
K = 32
WD = 4
F32 = jnp.float32
BF16 = jnp.bfloat16
MESH = pl.DeviceIdType.MESH
LOG2E = math.log2(math.e)


def split(x):
    high = x.astype(BF16)
    return high, (x - high.astype(F32)).astype(BF16)


def product(a, b, dims):
    return lax.dot_general(a, b, (dims, ((), ())), preferred_element_type=F32)


NN = ((1,), (0,))
NT = ((1,), (1,))
TN = ((0,), (0,))


def product3(a, b, dims=NN):
    ah, al = a
    bh, bl = b
    return product(ah, bh, dims) + product(ah, bl, dims) + product(al, bh, dims)


def iota(shape, dim):
    return lax.broadcasted_iota(jnp.int32, shape, dim)


def flag(cond):
    return jnp.full((8, 128), cond.astype(jnp.int32), jnp.int32) == 1


def splat(x):
    return jnp.broadcast_to(x, (8, 128))


def pick(mask, new, old):
    rows = new.shape[0]
    new3, old3 = new.reshape(rows // 8, 8, 128), old.reshape(rows // 8, 8, 128)
    return jnp.where(mask[None], new3, old3).reshape(rows, 128)


def kernel(
    planes,
    plane,
    cnt_hbm,
    jas_hbm,
    amp_hbm,
    inv_hbm,
    sla_hbm,
    pos_hbm,
    dis_hbm,
    mo_hbm,
    acc_hbm,
    cen_hbm,
    ex_hbm,
    orb_hbm,
    out,
    counts,
    jastrow,
    log_amp,
    inv,
    sla,
    pos,
    dis,
    mo,
    acc,
    cen,
    ex,
    orb,
    dhi,
    dlo,
    oh,
    oha,
    ac,
    misc,
    here,
    pts,
    logt,
    snd_a,
    part,
    rcv_a,
    rcv_b,
    solv,
    sla_r,
    sla_l,
    rs_r,
    rs_l,
    inv_r,
    inv_l,
    ri_r,
    ri_l,
    row_a,
    row_b,
    pre,
    tab_a,
    tab_b,
    in_sem,
    send_x,
    recv_x,
    send_a,
    recv_a,
    send_b,
    recv_b,
    up_sem,
):
    me = lax.axis_index("walkers")
    ob = lax.axis_index("orb")
    walkers = planes * plane
    core = ob % 2
    partner = (ob // 2) * 2 + (1 - core)
    across = (1 - ob // 2) * 2 + core
    z, r = me // plane, me % plane

    def at(w, o):
        return {"walkers": w, "orb": o}

    loads = [
        pltpu.make_async_copy(src, dst, in_sem.at[n])
        for n, (src, dst) in enumerate(
            (
                (mo_hbm, mo),
                (acc_hbm, acc),
                (pos_hbm, pos),
                (dis_hbm, dis),
                (cen_hbm, cen),
                (ex_hbm, ex),
                (cnt_hbm, counts),
                (jas_hbm, jastrow),
                (amp_hbm, log_amp),
                (orb_hbm, orb),
                (inv_hbm, inv),
                (sla_hbm, sla),
            )
        )
    ]
    for load in loads:
        load.start()
    barrier = pltpu.get_barrier_semaphore()

    def greet(w, o):
        pl.semaphore_signal(barrier, inc=1, device_id=at(w, o), device_id_type=MESH)

    greet(me, partner)
    greet(me, across)
    has_right, has_left = me < walkers - 1, me > 0

    @pl.when(has_right)
    def _():
        greet(me + 1, ob)

    @pl.when(has_left)
    def _():
        greet(me - 1, ob)

    for t in range(1, plane):
        greet(z * plane + (r + t) % plane, ob)

    for q in range(1, planes):
        @pl.when(q > z)
        def _(q=q):
            greet(q * plane + r, ob)

    @pl.when(me == 0)
    def _():
        rs_l[...] = jnp.zeros_like(rs_l)
        ri_l[...] = jnp.zeros_like(ri_l)

    @pl.when(me == walkers - 1)
    def _():
        rs_r[...] = jnp.zeros_like(rs_r)
        ri_r[...] = jnp.zeros_like(ri_r)

    late = z >= planes // 2
    early = jnp.logical_not(late)
    eager = late & (r >= 2)
    patient = jnp.logical_not(eager)

    def enter():
        neighbours = jnp.where(has_right, 1, 0) + jnp.where(has_left, 1, 0)
        pl.semaphore_wait(barrier, 2 + (plane - 1) + z + neighbours)

        @pl.loop(0, planes)
        def _(q):
            @pl.when(q < z)
            def _():
                pl.semaphore_signal(
                    up_sem.at[z],
                    inc=1,
                    device_id=at(q * plane + r, ob),
                    device_id_type=MESH,
                )

    for load in loads[:6]:
        load.wait()

    for w in range(WD):
        for c in range(3):
            for s in range(2):
                cols = slice(s * NEL, (s + 1) * NEL)
                n = 2 * c + s
                here[w, n : n + 1, :] = pos[c, w : w + 1, cols]
                here[w, n + 8 : n + 9, :] = dis[c, w : w + 1, cols]

    lane = iota((K, 128), 1)
    diag = lane == iota((K, 128), 0)

    @pl.loop(0, 2 * WD, unroll=4)
    def _(b):
        w, s = b // 2, b % 2
        order = mo[pl.ds(b, 1), :].astype(F32)
        taken = acc[pl.ds(b, 1), :].astype(F32)
        ek = jnp.sum(jnp.where(diag, order, 0.0), axis=1, keepdims=True)
        ak = jnp.sum(
            jnp.where(diag[:, :K], taken, 0.0), axis=1, keepdims=True
        )
        one = jnp.where(lane.astype(F32) == ek, 1.0, 0.0)
        took = one * ak
        rows = pl.ds(pl.multiple_of(b * K, K), K)
        oh[rows, :] = one.astype(BF16)
        oha[rows, :] = took.astype(BF16)
        ac[rows, :] = jnp.broadcast_to(ak, (K, 128))
        applied = jnp.sum(took, axis=0, keepdims=True)
        old, new = [], []
        for c in range(3):
            p = here[w, pl.ds(2 * c + s, 1), :]
            d = here[w, pl.ds(2 * c + s + 8, 1), :]
            old.append(jnp.sum(one * p, axis=1, keepdims=True))
            new.append(jnp.sum(one * (p + d), axis=1, keepdims=True))
            misc[w, pl.ds(2 * c + s, 1), :] = p + d * applied
        for c in range(3):
            pts[c, rows, :] = jnp.broadcast_to(old[c], (K, 128))
            pts[c + 3, rows, :] = jnp.broadcast_to(new[c], (K, 128))

    for load in loads[6:9]:
        load.wait()
    sub32 = iota((32, 128), 0)

    l1 = iota((1, 128), 1)
    c = [counts[n] for n in range(WD)]
    limit = [c[0]]
    for n in range(1, WD):
        limit.append(limit[-1] + c[n])
    start = [limit[n] - c[n] for n in range(WD)]
    total = limit[-1]
    def columns(ref, w, si, n):
        on = lane == sub32 + 32 * n
        got = []
        for c in range(3):
            row = ref[w, 2 * c + si : 2 * c + si + 1, :]
            got.append(jnp.sum(jnp.where(on, row, 0.0), axis=1, keepdims=True))
        return got

    def squares(column, ref, w, sj):
        out = jnp.zeros((32, 128), F32)
        for c in range(3):
            d = column[c] - ref[w, 2 * c + sj : 2 * c + sj + 1, :]
            out = out + d * d
        return out

    def whole(x):
        return jnp.sum(jnp.sum(x, axis=0, keepdims=True), axis=1, keepdims=True)

    def energies():
        @pl.loop(0, WD, unroll=True)
        def _(w):
            es = jnp.zeros((32, 128), F32)
            ed = jnp.zeros((32, 128), F32)
            for si in range(2):
                for n in range(4):
                    column = columns(misc, w, si, n)
                    es = es + lax.rsqrt(squares(column, misc, w, si) + 1.0)
                    if si == 0:
                        ed = ed + lax.rsqrt(squares(column, misc, w, 1) + 1.0)
            energy = (whole(es + 2.0 * ed) - 2.0 * NEL) / (2.0 * NEL * (2 * NEL - 1))
            misc[w, 6:7, :] = jnp.broadcast_to(energy, (1, 128))

        weighted = jnp.zeros((1, 128), F32)
        for n in range(WD):
            weighted = weighted + c[n].astype(F32) * misc[n, 6:7, :]
        own = jnp.where(l1 == 0, total.astype(F32), jnp.where(l1 == 1, weighted, 0.0))
        row_a[...] = own

    def jastrow_change():
        @pl.loop(0, WD)
        def _(w):
            def change_of(oc, nc, sj, falloff):
                od = jnp.sqrt(squares(oc, here, w, sj))
                nd = jnp.sqrt(squares(nc, misc, w, sj))
                return (nd - od) / ((1.0 + falloff * nd) * (1.0 + falloff * od))

            js = jnp.zeros((32, 128), F32)
            jd = jnp.zeros((32, 128), F32)
            for si in range(2):
                for n in range(4):
                    oc, nc = columns(here, w, si, n), columns(misc, w, si, n)
                    js = js + change_of(oc, nc, si, jastrow[2])
                    if si == 0:
                        jd = jd + change_of(oc, nc, 1, jastrow[3])
            jt = whole(jastrow[0] * js + (2.0 * jastrow[1]) * jd)
            misc[w, 7:8, :] = jnp.broadcast_to(jt, (1, 128))

    def in_plane(q):
        return pltpu.make_async_remote_copy(
            src_ref=row_a,
            dst_ref=tab_a.at[r],
            send_sem=send_a.at[q],
            recv_sem=recv_a.at[r],
            device_id=at(z * plane + q, ob),
            device_id_type=MESH,
        )

    def from_plane(q):
        return pltpu.make_async_remote_copy(
            src_ref=row_a,
            dst_ref=tab_a.at[q],
            send_sem=send_a.at[q],
            recv_sem=recv_a.at[q],
            device_id=at(z * plane + q, ob),
            device_id_type=MESH,
        )

    def send_plane():
        @pl.loop(1, plane)
        def _(t):
            in_plane((r + t) % plane).start()


    def table(tab, rows, place, own_row):
        before = jnp.zeros((1, 128), F32)
        every = jnp.zeros((1, 128), F32)
        for n in range(rows):
            x = jnp.where(jnp.full((1, 128), place, jnp.int32) == n, own_row, tab[n])
            before = before + jnp.where(jnp.full((1, 128), place, jnp.int32) > n, x, 0.0)
            every = every + x
        return before, every

    def in_column(q, slot):
        return pltpu.make_async_remote_copy(
            src_ref=row_b,
            dst_ref=tab_b.at[slot],
            send_sem=send_b.at[q],
            recv_sem=recv_b.at[slot],
            device_id=at(q * plane + r, ob),
            device_id_type=MESH,
        )

    def send_column():
        @pl.loop(1, plane)
        def _(t):
            from_plane((r + t) % plane).wait_recv()

        pre[...], row_b[...] = table(tab_a, plane, r, row_a[...])

        @pl.loop(0, planes)
        def _(q):
            @pl.when(q < z)
            def _():
                in_column(q, z).start()

    energies()

    @pl.when(eager)
    def _():
        enter()
        send_plane()

    loads[9].wait()
    shift = [jnp.zeros((128, 128), F32)] * 2
    for m in range(4):
        for b in range(2 * WD):
            w, s = b // 2, b % 2
            rows, to = slice(b * K, (b + 1) * K), slice(w * K, (w + 1) * K)
            for n in (2 * m, 2 * m + 1):
                span = slice(n * 128, (n + 1) * 128)
                rate = ex[n : n + 1, :] * (-LOG2E)
                far = jnp.zeros((K, 128), F32)
                near = jnp.zeros((K, 128), F32)
                for c3 in range(3):
                    center = cen[c3 : c3 + 1, span]
                    a, e = pts[c3, rows, :] - center, pts[c3 + 3, rows, :] - center
                    far = far + a * a
                    near = near + e * e
                high, low = split(jnp.exp2(rate * near) - jnp.exp2(rate * far))
                dhi[s, to, span] = high
                dlo[s, to, span] = low
        span = slice(m * 256, (m + 1) * 256)
        for s in range(2):
            high, low = split(orb[s, :, span])
            high4 = jnp.concatenate([high] * 4, axis=0)
            low4 = jnp.concatenate([low] * 4, axis=0)
            a = dhi[s, :, span]
            part_sum = product(a, high4, NT) + product(a, low4, NT)
            shift[s] = shift[s] + (part_sum + product(dlo[s, :, span], high4, NT))

    @pl.when(patient)
    def _():
        enter()
        send_plane()

    seg = iota((K, 128), 1) // K

    def block_rows(parts):
        return jnp.concatenate(
            [jnp.where(seg == n, x, 0.0) for n, x in enumerate(parts)], axis=0
        )

    shift_blocks = []
    for g in range(2):
        shift_blocks.append(
            split(
                block_rows(
                    [
                        shift[b % 2][(2 * g + b // 2) * K : (2 * g + b // 2 + 1) * K]
                        for b in range(4)
                    ]
                )
            )
        )

    loads[10].wait()
    change = []
    for g in range(2):
        rows = slice(g * 128, (g + 1) * 128)
        full = product3(shift_blocks[g], split(inv[rows, :]))
        change.append(jnp.where(ac[rows, :] > 0.5, full, 0.0))
    first = core == 0
    mine_mask = flag(first)
    snd_a[...] = pick(mine_mask, change[1], change[0])
    part[...] = pick(mine_mask, change[0], change[1])

    def remote(src, dst, n, w, o):
        return pltpu.make_async_remote_copy(
            src_ref=src,
            dst_ref=dst,
            send_sem=send_x.at[n],
            recv_sem=recv_x.at[n],
            device_id=at(w, o),
            device_id_type=MESH,
        )

    to_partner = remote(snd_a, rcv_a, 0, me, partner)

    to_partner.start()

    loads[11].wait()
    sla_now = []
    for g in range(2):
        rows = slice(g * 128, (g + 1) * 128)
        high, low = shift_blocks[g]
        taken = oha[rows, :]
        added = product(high, taken, TN) + product(low, taken, TN)
        sla[rows, :] = sla[rows, :] + added

    to_partner.wait_recv()
    part[...] = part[...] + rcv_a[...]
    to_across = remote(part, rcv_b, 1, me, across)
    to_across.start()

    @pl.when(late & (r >= 2))
    def _():
        send_column()

    jastrow_change()

    tiles = [misc[n] for n in range(WD)]

    def copy_masks(j):
        return [flag((start[n] <= j) & (j < limit[n])) for n in range(WD)]

    right_masks = [copy_masks(total - 1), copy_masks(total - 2)]
    left_masks = [copy_masks(jnp.int32(0)), copy_masks(jnp.int32(1))]

    def chosen(masks, parts):
        out = jnp.zeros_like(parts[0])
        for m, x in zip(masks, parts):
            out = pick(m, x, out)
        return out

    def pack(dst, masks, parts, n_rows):
        for n in range(2):
            dst[n * n_rows : (n + 1) * n_rows, :] = chosen(masks[n], parts)

    slaters = [sla[n * 64 : (n + 1) * 64, :] for n in range(WD)]
    pack(sla_r, right_masks, slaters, 64)
    pack(sla_l, left_masks, slaters, 64)
    for n in range(2):
        sla_r[128 + 8 * n : 136 + 8 * n, :] = chosen(right_masks[n], tiles)
        sla_l[128 + 8 * n : 136 + 8 * n, :] = chosen(left_masks[n], tiles)

    column_blocks = []
    block_on = (iota((128, 128), 0) // K) == (iota((128, 128), 1) // K)
    for g in range(2):
        rows = slice(g * 128, (g + 1) * 128)
        high, low = split(inv[rows, :])
        which = oh[rows, :]
        got = product(high, which, NT) + product(low, which, NT)
        column_blocks.append(split(jnp.where(block_on, got, 0.0)))

    slater_right = remote(sla_r, rs_l, 3, me + 1, ob)
    slater_left = remote(sla_l, rs_r, 4, me - 1, ob)

    def start_both(to_right, to_left):
        @pl.when(has_right)
        def _():
            to_right.start()

        @pl.when(has_left)
        def _():
            to_left.start()

    @pl.when(late & (r < 2))
    def _():
        send_column()

    to_across.wait_recv()
    start_both(slater_right, slater_left)
    summed = part[...] + rcv_b[...]
    high, low = split(summed)
    which = oh[pl.ds(pl.multiple_of(core * 128, 128), 128), :]
    got = product(high, which, NT) + product(low, which, NT)
    lane8 = iota((8, 128), 1)
    sub8 = iota((8, 128), 0)
    seg8 = lane8 // K
    in_seg = lane8 % K
    tile = []
    for t in range(4):
        x = jnp.where(in_seg == sub8 + 8 * t, 1.0, 0.0)
        for b in range(4):
            x = x + jnp.where(seg8 == b, got[b * K + 8 * t : b * K + 8 * t + 8], 0.0)
        tile.append(x)

    def panel(p, carry):
        m, logs = list(carry[:4]), carry[4]
        base = 8 * p
        cols = [
            [jnp.take_along_axis(m[t], seg8 * K + base + n, axis=1) for t in range(4)]
            for n in range(8)
        ]
        pivots = jnp.ones((8, 128), F32)
        for n in range(8):
            bk = cols[n]
            pivot = bk[0][n : n + 1, :]
            inverse_pivot = 1.0 / pivot
            pivots = jnp.where(sub8 == n, pivot, pivots)
            spot = in_seg == base + n
            row = jnp.where(spot, inverse_pivot, m[0][n : n + 1, :] * inverse_pivot)
            for t in range(4):
                fresh = jnp.where(spot, 0.0, m[t]) - bk[t] * row
                m[t] = jnp.where(sub8 == n, row, fresh) if t == 0 else fresh
            for j in range(n + 1, 8):
                scale = cols[j][0][n : n + 1, :] * inverse_pivot
                for t in range(4):
                    fresh = cols[j][t] - bk[t] * scale
                    cols[j][t] = jnp.where(sub8 == n, scale, fresh) if t == 0 else fresh
        logs = logs + jnp.log(jnp.abs(pivots))
        return m[1], m[2], m[3], m[0], logs

    *tile, logs = lax.fori_loop(0, 4, panel, (*tile, jnp.zeros((8, 128), F32)))
    reverse = jnp.concatenate(tile, axis=0)
    solved = product3(split(block_rows([reverse] * 4)), (high, low))
    logdet = jnp.broadcast_to(jnp.sum(logs, axis=0, keepdims=True), (8, 128))
    solv[core, 0:128, :] = solved
    solv[core, 128:136, :] = logdet
    swap = remote(solv.at[core], solv.at[core], 2, me, partner)
    swap.start()

    @pl.when(early)
    def _():
        send_column()

    swap_in = remote(solv.at[1 - core], solv.at[1 - core], 2, me, partner)
    swap_in.wait_recv()
    for g in range(2):
        rows = slice(g * 128, (g + 1) * 128)
        inv[rows, :] = inv[rows, :] - product3(column_blocks[g], split(solv[g, 0:128, :]))
    for n in range(WD):
        row = solv[n // 2, 128:136, :]
        base = 64 * (n % 2)
        up_down = jnp.where((lane8 == base) | (lane8 == base + K), row, 0.0)
        both = splat(jnp.sum(up_down, axis=1, keepdims=True))
        logt[8 * n : 8 * n + 8, :] = (log_amp[n] + both) + 0.5 * splat(tiles[n][7:8, :])
    inverses = [inv[n * 64 : (n + 1) * 64, :] for n in range(WD)]
    log_tiles = [logt[8 * n : 8 * n + 8, :] for n in range(WD)]
    pack(inv_r, right_masks, inverses, 64)
    pack(inv_l, left_masks, inverses, 64)
    for n in range(2):
        inv_r[128 + 8 * n : 136 + 8 * n, :] = chosen(right_masks[n], log_tiles)
        inv_l[128 + 8 * n : 136 + 8 * n, :] = chosen(left_masks[n], log_tiles)
    inverse_right = remote(inv_r, ri_l, 5, me + 1, ob)
    inverse_left = remote(inv_l, ri_r, 6, me - 1, ob)
    start_both(inverse_right, inverse_left)

    @pl.loop(1, planes)
    def _(t):
        @pl.when(z + t < planes)
        def _():
            pl.semaphore_wait(up_sem.at[z + t], 1)
            in_column(z + t, z).start()

    for copy in (
        to_partner,
        to_across,
        swap,
    ):
        copy.wait_send()

    @pl.loop(1, plane)
    def _(t):
        in_plane((r + t) % plane).wait_send()

    @pl.loop(1, planes)
    def _(t):
        q = (z + t) % planes
        in_column(q, q).wait_recv()

    @pl.loop(1, planes)
    def _(t):
        in_column((z + t) % planes, z).wait_send()

    every_a, before_a = row_b[...], pre[...]

    before_b, every_b = table(tab_b, planes, z, every_a)
    mean = jnp.sum(jnp.where(l1 == 1, every_b, 0.0), axis=1, keepdims=True)
    out[552:560, :] = splat(mean) / (WD * walkers)
    ahead = jnp.where(l1 == 0, before_a + before_b, 0.0)
    over = splat(jnp.sum(ahead, axis=1, keepdims=True)) - (WD * me).astype(F32)

    @pl.when(has_left)
    def _():
        slater_right.wait_recv()
        inverse_right.wait_recv()

    @pl.when(has_right)
    def _():
        slater_left.wait_recv()
        inverse_left.wait_recv()

    totalf = total.astype(F32)
    for i in range(WD):
        j = i - over
        masks = [j == -1.0, j == -2.0]
        masks += [
            (j >= start[n].astype(F32)) & (j < limit[n].astype(F32)) for n in range(WD)
        ]
        masks += [j == totalf, j == totalf + 1.0]

        def halo(ref_l, ref_r, n_rows, base):
            return [ref_l[base + n * n_rows : base + (n + 1) * n_rows, :] for n in range(2)], [
                ref_r[base + n * n_rows : base + (n + 1) * n_rows, :] for n in range(2)
            ]

        def select(own_parts, ref_l, ref_r, n_rows, base):
            a, e = halo(ref_l, ref_r, n_rows, base)
            return chosen(masks, a + own_parts + e)

        out[i * 64 : (i + 1) * 64, :] = select(
            [inv[n * 64 : (n + 1) * 64, :] for n in range(WD)], ri_l, ri_r, 64, 0
        )
        out[256 + i * 64 : 256 + (i + 1) * 64, :] = select(
            [sla[n * 64 : (n + 1) * 64, :] for n in range(WD)], rs_l, rs_r, 64, 0
        )
        small = select([misc[n] for n in range(WD)], rs_l, rs_r, 8, 128)
        logs_here = select(
            [logt[8 * n : 8 * n + 8, :] for n in range(WD)], ri_l, ri_r, 8, 128
        )
        for n in range(6):
            row = 512 + 4 * n + i
            out[row : row + 1, :] = small[n : n + 1, :]
        out[536 + i : 537 + i, :] = logs_here[0:1, :]
        out[544 + i : 545 + i, :] = small[6:7, :]

    @pl.when(has_right)
    def _():
        slater_right.wait_send()
        inverse_right.wait_send()

    @pl.when(has_left)
    def _():
        slater_left.wait_send()
        inverse_left.wait_send()


def finish(packed, out_inv, out_sla, out_pos, out_log, out_en, out_mean):
    out_inv[...] = packed[0:256, :]
    out_sla[...] = packed[256:512, :]
    for c in range(3):
        for s in range(2):
            row = 512 + 8 * c + 4 * s
            out_pos[c, :, s * NEL : (s + 1) * NEL] = packed[row : row + 4, :]
    logs, energies = packed[536:544, :], packed[544:552, :]
    for i in range(WD):
        out_log[i] = logs[i, 0]
        out_en[i] = energies[i, 0]
    out_mean[0] = packed[552:560, :][0, 0]


def solution(mesh):
    walkers = mesh.shape["walkers"]
    plane = 16 if walkers == 128 else walkers // 2
    planes = walkers // plane

    def body(
        inverse,
        slater,
        positions,
        displacements,
        move_order,
        accepted,
        counts,
        log_amp,
        centers,
        exponents,
        orbitals,
        jastrow,
    ):
        smem = pl.BlockSpec(memory_space=pltpu.SMEM)
        vmem = pl.BlockSpec(memory_space=pltpu.VMEM)
        hbm = pl.BlockSpec(memory_space=pltpu.HBM)

        def shape(*dims):
            return jax.ShapeDtypeStruct(dims, F32)

        def buf(*dims, kind=F32):
            return pltpu.VMEM(dims, kind)

        dma = pltpu.SemaphoreType.DMA
        packed = pl.pallas_call(
            lambda *refs: kernel(planes, plane, *refs),
            out_shape=shape(560, 128),
            in_specs=[hbm] * 12,
            out_specs=vmem,
            scratch_shapes=[
                pltpu.SMEM((4,), jnp.int32),
                pltpu.SMEM((4,), F32),
                pltpu.SMEM((4,), F32),
                buf(256, 128),
                buf(256, 128),
                buf(3, 4, 256),
                buf(3, 4, 256),
                buf(8, 128, kind=jnp.int32),
                buf(8, 32, kind=jnp.int32),
                buf(3, 1024),
                buf(8, 128),
                buf(2, 32, 1024),
                buf(2, 128, 1024, kind=BF16),
                buf(2, 128, 1024, kind=BF16),
                buf(256, 128, kind=BF16),
                buf(256, 128, kind=BF16),
                buf(256, 128),
                buf(4, 8, 128),
                buf(4, 16, 128),
                buf(6, 256, 128),
                buf(32, 128),
                buf(128, 128),
                buf(128, 128),
                buf(128, 128),
                buf(128, 128),
                buf(2, 136, 128),
                *[buf(144, 128) for _ in range(8)],
                buf(1, 128),
                buf(1, 128),
                buf(1, 128),
                buf(plane, 1, 128),
                buf(planes, 1, 128),
                dma((12,)),
                dma((7,)),
                dma((7,)),
                dma((plane,)),
                dma((plane,)),
                dma((planes,)),
                dma((planes,)),
                pltpu.SemaphoreType.REGULAR((planes,)),
            ],
            compiler_params=pltpu.CompilerParams(
                collective_id=0, has_side_effects=True, vmem_limit_bytes=16 << 20
            ),
            name="generation",
        )(*[pltpu.with_memory_space_constraint(x, pltpu.HBM) for x in (
            counts,
            jastrow,
            log_amp,
            inverse.reshape(256, 128),
            slater.reshape(256, 128),
            positions.transpose(1, 0, 2),
            displacements.transpose(1, 0, 2),
            move_order.reshape(8, 128),
            accepted.reshape(8, 32),
            centers,
            exponents.reshape(8, 128),
            orbitals,
        )])
        outs = pl.pallas_call(
            finish,
            out_shape=(
                shape(256, 128),
                shape(256, 128),
                shape(3, 4, 256),
                shape(4),
                shape(4),
                shape(1),
            ),
            in_specs=[vmem],
            out_specs=(vmem, vmem, vmem, smem, smem, smem),
            compiler_params=pltpu.CompilerParams(vmem_limit_bytes=4 << 20),
            name="finish",
        )(packed)
        return (
            outs[0].reshape(4, 2, 32, 128),
            outs[1].reshape(4, 2, 32, 128),
            outs[2].transpose(1, 0, 2),
            outs[3],
            outs[4],
            outs[5].reshape(()),
        )

    placed = (
        P("walkers", None, "orb", None),
        P("walkers", None, "orb", None),
        P("walkers", None, None),
        P("walkers", None, None),
        P("walkers", None, None),
        P("walkers", None, None),
        P("walkers"),
        P("walkers"),
        P(),
        P(),
        P(None, "orb", None),
        P(),
    )
    return jax.shard_map(
        body,
        mesh=mesh,
        in_specs=placed,
        out_specs=(
            P("walkers", None, "orb", None),
            P("walkers", None, "orb", None),
            P("walkers", None, None),
            P("walkers"),
            P("walkers"),
            P(),
        ),
        check_vma=False,
    )
```
